32 devices in a mesh: station: 4 (over y, x), dom: 8 (over z, core).
Axes of the slice: x: 2, y: 2, z: 4, core: 2. Of those that a mesh axis runs over, the one named last changes fastest.
Arguments:
- beam_first: float32 [4, 8, 4, 8192], P('station', 'dom'), may hold values from -3.5 to 3.5
- beam_second: float32 [4, 8, 4, 8192], P('station', 'dom'), may hold values from -3.5 to 3.5
- green_smooth: float32 [128, 128], replicated, may hold values from -0.5 to 0.5
- green_slope: float32 [128, 128], replicated, may hold values from -0.5 to 0.5
- destination: int32 [4, 512, 1], P('station', 'dom'), may hold values from 0 to 3; in each aligned block of 64 rows (0 to 63, 64 to 127, ..., all dimensions but the last counted through in order) at most 32 rows name the same one
Outputs:
- resliced: float32 [4, 8, 4, 32, 4, 128], P('station', 'dom')
- beam_second_out: float32 [4, 8, 4, 8192], P('station', 'dom')
The draws below stay inside these ranges and needn't reach their ends.
Inputs may be any that keep to these rules, and one draw needn't show every extreme that they name: `destination`: in the rows of one device (the 64 blocks of one station and dom index) no station is named more than 32 times, a bound that some block reaches.
All inputs are finite; a program needn't handle non-finite values.
Results may differ from the reference program's by a relative error of at most 0.00095.
Values may be sent and summed in bfloat16 or wider, within the bound.
No kernel may reach another device: no remote copies, remote signals or barrier semaphores. Data moves between devices by JAX's collectives and lax.ppermute only.
A program may use at most 64 MiB of HBM per device.

```python
import math
import jax
import jax.numpy as jnp
import numpy as np
from jax import lax

GRID = 128
NPD = 8192
FRONTS = 4
BLOCK = 128
STATIONS = 4
DOMS = 8
BLK = 64
CAP = 32


def particle_draw(key, salt):
    key = jax.random.fold_in(key, salt)
    key_core, key_wide, key_pick, key_moment = jax.random.split(key, 4)
    shape = (2, STATIONS, DOMS, NPD)
    core = jnp.clip(jax.random.normal(key_core, shape, jnp.float32), -3.5, 3.5)
    moment = jnp.clip(jax.random.normal(key_moment, shape, jnp.float32), -3.5, 3.5)
    share = 0.5
    wide = jax.random.uniform(key_wide, shape, jnp.float32, -3.5, 3.5)
    picked = jax.random.uniform(key_pick, shape, jnp.float32) < share
    position = jnp.where(picked, wide, core)
    return jnp.stack([position[0], moment[0], position[1], moment[1]], axis=2).astype(jnp.float32)


def draw_beam_first(key, part):
    return particle_draw(key, 101)


def draw_beam_second(key, part):
    return particle_draw(key, 202)


def deal_out(stream_key, own, number, rows, count, top, most, lean):
    order = jax.random.permutation(stream_key, count)
    packed, usual = portions_of(count, rows * top, most, lean, True), portions_of(count, rows * top, most, lean, False)
    places = jnp.arange(count)

    def named(lengths, rotation):
        used = int((lengths > 0).sum())
        fixed = max(1, used // 4)
        passed = fixed + (places - fixed + rotation * (used - fixed)) % max(1, count - fixed)
        return jnp.zeros((count,), jnp.int32).at[order[jnp.where(places < fixed, places, passed)]].set(jnp.asarray(lengths, jnp.int32))

    lengths = jnp.where(number % 4 == 0, named(packed, number // 4), named(usual, number - number // 4 - 1))
    mixed = jax.random.permutation(jax.random.fold_in(own, 3), count)
    donor, receiver = mixed[0:count // 2 * 2:2], mixed[1:count // 2 * 2:2]
    room = jnp.minimum(lengths[donor] - 1, most - lengths[receiver]) // 2
    room = jnp.where((donor == order[0]) | (receiver == order[0]) | (lengths[receiver] == 0), 0, jnp.maximum(room, 0))
    passed = jax.random.randint(jax.random.fold_in(own, 4), (count // 2,), 0, 1 << 20) % (room + 1)
    lengths = lengths.at[donor].add(-passed).at[receiver].add(passed)
    labels = jnp.searchsorted(jnp.cumsum(lengths), jnp.arange(rows * top), side="right").astype(jnp.int32)
    listing = labels.reshape(top, rows).T
    listing = listing[jax.random.permutation(jax.random.fold_in(own, 1), rows)]
    rotation = jax.random.randint(jax.random.fold_in(own, 2), (rows, 1), 0, top)
    return jnp.take_along_axis(listing, (jnp.arange(top)[None, :] + rotation) % top, axis=1)


def portions_of(number_of, total, bound, slope, full):
    portions = [(1 << 20) // math.isqrt(standing ** slope) + 1 for standing in range(1, number_of + 1)]
    largest = bound if full else min(bound, max(-(-total // number_of), total * portions[0] // sum(portions)))
    least = 1 if total - largest >= number_of - 1 else 0
    counts, rest = [largest] + [least] * (number_of - 1), total - largest - least * (number_of - 1)
    while rest > 0:
        candidates = [i for i in range(1, number_of) if counts[i] < largest] or [i for i in range(1, number_of) if counts[i] < bound]
        mass, left = sum([portions[i] for i in candidates]), rest
        for i in candidates:
            more = min(bound - counts[i], max(1, left * portions[i] // mass), rest)
            counts[i] = counts[i] + more
            rest = rest - more
    return np.array(counts)


def gaussian(stream_key, extent, spread, most, kind=jnp.bfloat16):
    return jnp.clip(spread * jax.random.normal(stream_key, extent, jnp.float32), -most, most).astype(kind)


def setup_inputs(seed: int = 0) -> dict:
    streams_of = jax.random.split(jax.random.key(seed), 6)
    beam_first = draw_beam_first(jax.random.fold_in(streams_of[5], 71), 0)
    beam_second = draw_beam_second(jax.random.fold_in(streams_of[5], 71), 0)
    green_smooth = gaussian(streams_of[2], (GRID, GRID), GRID ** -0.5, 0.5, jnp.float32)
    green_slope = gaussian(streams_of[3], (GRID, GRID), GRID ** -0.5, 0.5, jnp.float32)
    destination_keys = jax.random.split(jax.random.fold_in(streams_of[4], 1), STATIONS * (DOMS * BLK) // BLK)
    destination_turns = jax.random.permutation(jax.random.fold_in(streams_of[4], 3), STATIONS * (DOMS * BLK) // BLK)
    destination = jax.vmap(lambda own, number: deal_out(jax.random.fold_in(streams_of[4], 2), own, number, BLK, STATIONS, 1, CAP, 2))(destination_keys, destination_turns).reshape((STATIONS, DOMS * BLK, 1))
    return dict(beam_first=beam_first, beam_second=beam_second, green_smooth=green_smooth, green_slope=green_slope, destination=destination)


EDGE = 4.0
DRIFT = 0.05
STRENGTH = 0.06
HIGH = lax.Precision.HIGHEST


def hat_table(coordinate):
    spacing = 2.0 * EDGE / (GRID - 1)
    centers = -EDGE + spacing * jnp.arange(GRID).astype(jnp.float32)
    weights = jnp.maximum(0.0, 1.0 - jnp.abs(coordinate[:, None] - centers[None, :]) / spacing)
    return weights.astype(jnp.bfloat16)


def deposit(particles):
    hat_x = hat_table(particles[0])
    hat_y = hat_table(particles[2])
    return lax.dot_general(hat_x, hat_y, (((0,), (0,)), ((), ())), preferred_element_type=jnp.float32)


def field_table(density, green_smooth, green_slope):
    first = jnp.dot(density, green_smooth.T, precision=HIGH)
    second = jnp.dot(density, green_slope.T, precision=HIGH)
    return jnp.concatenate([jnp.dot(green_slope, first, precision=HIGH), jnp.dot(green_smooth, second, precision=HIGH)], axis=1).astype(jnp.bfloat16)


def kick_drift(particles, table):
    hat_x = hat_table(particles[0])
    hat_y = hat_table(particles[2])
    sampled = jnp.dot(hat_x, table, preferred_element_type=jnp.float32)
    weight_y = hat_y.astype(jnp.float32)
    push_x = jnp.sum(sampled[:, :GRID] * weight_y, axis=1)
    push_y = jnp.sum(sampled[:, GRID:] * weight_y, axis=1)
    moment_x = particles[1] - push_x
    moment_y = particles[3] - push_y
    return jnp.stack([particles[0] + DRIFT * moment_x, moment_x, particles[2] + DRIFT * moment_y, moment_y])


def pack_blocks(particles, routes, stations, capacity):
    onehot = (routes[:, None] == jnp.arange(stations, dtype=jnp.int32)[None, :]).astype(jnp.int32)
    ranking = jnp.sum((jnp.cumsum(onehot, axis=0) - onehot) * onehot, axis=1).astype(jnp.int32)
    target = jnp.arange(stations * capacity, dtype=jnp.int32)
    placing = ((routes[None, :] == (target // capacity)[:, None]) & (ranking[None, :] == (target % capacity)[:, None])).astype(particles.dtype)
    blocks = particles.reshape(4, -1, BLOCK)
    return jnp.einsum("rb,kbc->rkc", placing, blocks, precision=HIGH)


def reference(beam_first, beam_second, green_smooth, green_slope, destination):
    density_scale = STRENGTH * GRID * GRID / (NPD * DOMS)

    def station_front(paired):
        first_slice, second_slice = paired
        dens_first = jnp.sum(jax.vmap(deposit)(first_slice), axis=0) * density_scale
        dens_second = jnp.sum(jax.vmap(deposit)(second_slice), axis=0) * density_scale
        table_first = field_table(dens_first, green_smooth, green_slope)
        table_second = field_table(dens_second, green_smooth, green_slope)
        moved_first = jax.vmap(kick_drift, in_axes=(0, None))(first_slice, table_second)
        moved_second = jax.vmap(kick_drift, in_axes=(0, None))(second_slice, table_first)
        return moved_first, moved_second

    for front_index in range(FRONTS):
        beam_first, beam_second = lax.map(station_front, (beam_first, beam_second))
        if front_index + 1 < FRONTS:
            beam_second = jnp.roll(beam_second, 1, axis=0)
    routes = destination.reshape(STATIONS, DOMS, BLK).astype(jnp.int32)
    packer = lambda particles, route_row: pack_blocks(particles, route_row, STATIONS, CAP)
    sent = jax.vmap(jax.vmap(packer))(beam_first, routes)
    sent = sent.reshape(STATIONS, DOMS, STATIONS, CAP, 4, BLOCK)
    return jnp.transpose(sent, (2, 1, 0, 3, 4, 5)), beam_second
```

```python
import jax
import jax.numpy as jnp
from jax import lax
from jax.sharding import PartitionSpec as P

GRID = 128
FRONTS = 4
BLOCK = 128


EDGE = 4.0
DRIFT = 0.05
STRENGTH = 0.06
HIGH = lax.Precision.HIGHEST


def shifted(value, axis, steps):
    count = lax.axis_size(axis)
    pairs = [(source, (source + steps) % count) for source in range(count)]
    return lax.ppermute(value, axis, pairs)


def summed(value, axis):
    count = lax.axis_size(axis)
    step = 1
    while step < count:
        pairs = [(source, source ^ step) for source in range(count)]
        value = value + lax.ppermute(value.astype(jnp.bfloat16), axis, pairs).astype(jnp.float32)
        step *= 2
    return value


def hat_table(coordinate):
    spacing = 2.0 * EDGE / (GRID - 1)
    centers = -EDGE + spacing * jnp.arange(GRID).astype(jnp.float32)
    weights = jnp.maximum(0.0, 1.0 - jnp.abs(coordinate[:, None] - centers[None, :]) / spacing)
    return weights.astype(jnp.bfloat16)


def deposit(hat_x, hat_y):
    return lax.dot_general(
        hat_x, hat_y, (((0,), (0,)), ((), ())), preferred_element_type=jnp.float32
    )


def finish_table(inner_smooth, inner_slope, green_smooth, green_slope):
    return jnp.concatenate(
        [
            jnp.dot(green_slope, inner_smooth, precision=HIGH),
            jnp.dot(green_smooth, inner_slope, precision=HIGH),
        ],
        axis=1,
    ).astype(jnp.bfloat16)


def kick_drift(particles, hat_x, hat_y, table):
    sampled = jnp.dot(hat_x, table, preferred_element_type=jnp.float32)
    weight_y = hat_y.astype(jnp.float32)
    push_x = jnp.sum(sampled[:, :GRID] * weight_y, axis=1)
    push_y = jnp.sum(sampled[:, GRID:] * weight_y, axis=1)
    moment_x = particles[1] - push_x
    moment_y = particles[3] - push_y
    return jnp.stack(
        [particles[0] + DRIFT * moment_x, moment_x, particles[2] + DRIFT * moment_y, moment_y]
    )


def pack_blocks(particles, routes, stations, capacity):
    onehot = (routes[:, None] == jnp.arange(stations, dtype=jnp.int32)[None, :]).astype(jnp.int32)
    ranking = jnp.sum((jnp.cumsum(onehot, axis=0) - onehot) * onehot, axis=1)
    target = jnp.arange(stations * capacity, dtype=jnp.int32)
    placing = (
        (routes[None, :] == (target // capacity)[:, None])
        & (ranking[None, :] == (target % capacity)[:, None])
    ).astype(particles.dtype)
    blocks = particles.reshape(4, -1, BLOCK)
    return jnp.einsum("rb,kbc->rkc", placing, blocks, precision=HIGH)


def shards(beam_first, beam_second, green_smooth, green_slope, destination):
    resident = beam_first[0, 0]
    opposing = beam_second[0, 0]
    groups = lax.axis_size("dom")
    stations = lax.axis_size("station")
    density_scale = STRENGTH * GRID * GRID / (resident.shape[1] * groups)
    for front_index in range(FRONTS):
        hat_rx = hat_table(resident[0])
        hat_ry = hat_table(resident[2])
        hat_ox = hat_table(opposing[0])
        hat_oy = hat_table(opposing[2])
        part_resident = deposit(hat_rx, hat_ry)
        part_opposing = deposit(hat_ox, hat_oy)
        dens_resident, dens_opposing = summed(jnp.stack([part_resident, part_opposing]), "dom")
        dens_resident = dens_resident * density_scale
        dens_opposing = dens_opposing * density_scale
        smooth_res = jnp.dot(dens_resident, green_smooth.T, precision=HIGH)
        slope_res = jnp.dot(dens_resident, green_slope.T, precision=HIGH)
        smooth_opp = jnp.dot(dens_opposing, green_smooth.T, precision=HIGH)
        slope_opp = jnp.dot(dens_opposing, green_slope.T, precision=HIGH)
        table_resident = finish_table(smooth_res, slope_res, green_smooth, green_slope)
        table_opposing = finish_table(smooth_opp, slope_opp, green_smooth, green_slope)
        resident = kick_drift(resident, hat_rx, hat_ry, table_opposing)
        opposing = kick_drift(opposing, hat_ox, hat_oy, table_resident)
        if front_index + 1 < FRONTS:
            opposing = shifted(opposing, "station", 1)
    block_count = resident.shape[1] // BLOCK
    capacity = max(2, 2 * block_count // stations)
    outgoing = pack_blocks(resident, destination[0, :, 0], stations, capacity)
    outgoing = outgoing.reshape(stations, capacity, 4, BLOCK)
    arrived = lax.all_to_all(outgoing, "station", split_axis=0, concat_axis=0, tiled=True)
    return (arrived[None, None], opposing[None, None])


def solution(mesh):
    placed = (
        P("station", "dom", None, None),
        P("station", "dom", None, None),
        P(),
        P(),
        P("station", "dom", None),
    )
    return jax.shard_map(
        shards,
        mesh=mesh,
        in_specs=placed,
        out_specs=(P("station", "dom", None, None, None, None), P("station", "dom", None, None)),
        check_vma=False,
    )
```

```python
import functools

import jax
import jax.numpy as jnp
from jax import lax
from jax.experimental import pallas as pl
from jax.experimental.pallas import tpu as pltpu
from jax.sharding import PartitionSpec as P

GRID = 128
FRONTS = 4
BLOCK = 128
TILE = 4096
ROWS = 16


EDGE = 4.0
DRIFT = 0.05
STRENGTH = 0.06
HIGH = lax.Precision.HIGHEST
SPACING = 2.0 * EDGE / (GRID - 1)


def shifted(value, axis, steps):
    count = lax.axis_size(axis)
    pairs = [(source, (source + steps) % count) for source in range(count)]
    return lax.ppermute(value, axis, pairs)


def summed(value, axis):
    count = lax.axis_size(axis)
    step = 1
    while step < count:
        pairs = [(source, source ^ step) for source in range(count)]
        value = value + lax.ppermute(value.astype(jnp.bfloat16), axis, pairs).astype(jnp.float32)
        step *= 2
    return value


def hat_table(coordinate):
    count = coordinate.shape[1]
    place = jnp.clip((coordinate + EDGE) * (1.0 / SPACING), -2.0, GRID + 2.0)
    cell = jnp.floor(place)
    upper = place - cell
    lower = 1.0 - upper

    def spread(row):
        return jnp.broadcast_to(row, (ROWS, count)).astype(jnp.bfloat16)

    cell, lower, upper = spread(cell), spread(lower), spread(upper)
    none = jnp.zeros((ROWS, count), jnp.bfloat16)
    index = lax.broadcasted_iota(jnp.int32, (ROWS, count), 0).astype(jnp.float32)
    parts = []
    for start in range(0, GRID, ROWS):
        at = (index + float(start)).astype(jnp.bfloat16)
        before = (index + float(start - 1)).astype(jnp.bfloat16)
        parts.append(jnp.where(cell == at, lower, jnp.where(cell == before, upper, none)))
    return jnp.concatenate(parts, axis=0)


def deposit(x, y):
    return lax.dot_general(
        hat_table(y), hat_table(x), (((1,), (1,)), ((), ())), preferred_element_type=jnp.float32
    )


def kick(x, moment_x, y, moment_y, table):
    sampled = jnp.dot(table, hat_table(x), preferred_element_type=jnp.float32)
    weight_y = hat_table(y).astype(jnp.float32)
    moment_x = moment_x - jnp.sum(sampled[:GRID] * weight_y, axis=0, keepdims=True)
    moment_y = moment_y - jnp.sum(sampled[GRID:] * weight_y, axis=0, keepdims=True)
    return x + DRIFT * moment_x, moment_x, y + DRIFT * moment_y, moment_y


def tables(density, smooth, slope, scale):
    stacked = density.reshape(2 * GRID, GRID) * scale
    greens = jnp.concatenate([slope, smooth], axis=0)
    inner = lax.dot_general(
        stacked, greens, (((1,), (1,)), ((), ())), precision=HIGH, preferred_element_type=jnp.float32
    )
    by_slope = jnp.concatenate([inner[:GRID, :GRID], inner[GRID:, :GRID]], axis=1)
    by_smooth = jnp.concatenate([inner[:GRID, GRID:], inner[GRID:, GRID:]], axis=1)
    push_x = jnp.dot(smooth, by_slope, precision=HIGH, preferred_element_type=jnp.float32)
    push_y = jnp.dot(slope, by_smooth, precision=HIGH, preferred_element_type=jnp.float32)
    both = jnp.concatenate([push_x, push_y], axis=0).astype(jnp.bfloat16)
    return both[:, :GRID], both[:, GRID:]


def columns(count):
    width = min(TILE, count)
    return [pl.ds(start, width) for start in range(0, count, width)]


def first_kernel(resident_ref, opposing_ref, density_ref):
    for which, ref in enumerate((resident_ref, opposing_ref)):
        density_ref[which] = sum(
            deposit(ref[0:1, tile], ref[2:3, tile]) for tile in columns(ref.shape[1])
        )


def opposing_kernel(scale, split, density_ref, smooth_ref, slope_ref, *refs):
    own, other = tables(density_ref[...], smooth_ref[...], slope_ref[...], scale)
    *sources, place_ref, moment_ref, table_ref = refs
    table_ref[...] = other
    for tile in columns(place_ref.shape[1]):
        if split:
            x, y = (sources[0][row : row + 1, tile] for row in range(2))
            moment_x, moment_y = (sources[1][row : row + 1, tile] for row in range(2))
        else:
            x, moment_x, y, moment_y = (sources[0][row : row + 1, tile] for row in range(4))
        x, moment_x, y, moment_y = kick(x, moment_x, y, moment_y, own)
        place_ref[0:1, tile] = x
        place_ref[1:2, tile] = y
        moment_ref[0:1, tile] = moment_x
        moment_ref[1:2, tile] = moment_y


def resident_kernel(table_ref, beam_ref, moved_ref, density_ref):
    total = 0.0
    for tile in columns(beam_ref.shape[1]):
        new = kick(*(beam_ref[row : row + 1, tile] for row in range(4)), table_ref[...])
        for row in range(4):
            moved_ref[row : row + 1, tile] = new[row]
        total = total + deposit(new[0], new[2])
    density_ref[...] = total


def arrival_kernel(place_ref, resident_ref, density_ref):
    density_ref[0] = resident_ref[...]
    density_ref[1] = sum(
        deposit(place_ref[0:1, tile], place_ref[1:2, tile]) for tile in columns(place_ref.shape[1])
    )


def last_kernel(scale, slots_ref, density_ref, smooth_ref, slope_ref, beam_ref, packed_ref, table_ref, moved_ref):
    table_ref[...], other = tables(density_ref[...], smooth_ref[...], slope_ref[...], scale)
    packed_ref[...] = jnp.zeros_like(packed_ref)
    for tile in columns(beam_ref.shape[1]):
        new = kick(*(beam_ref[row : row + 1, tile] for row in range(4)), other)
        for row in range(4):
            moved_ref[row : row + 1, tile] = new[row]
    for block in range(beam_ref.shape[1] // BLOCK):
        packed_ref[slots_ref[block]] = moved_ref[:, block * BLOCK : (block + 1) * BLOCK]


def final_kernel(table_ref, place_ref, moment_ref, out_ref):
    for tile in columns(place_ref.shape[1]):
        new = kick(
            place_ref[0:1, tile],
            moment_ref[0:1, tile],
            place_ref[1:2, tile],
            moment_ref[1:2, tile],
            table_ref[...],
        )
        for row in range(4):
            out_ref[row : row + 1, tile] = new[row]


def local(kernel, out_shape, **options):
    return pl.pallas_call(
        kernel,
        out_shape=out_shape,
        compiler_params=pltpu.CompilerParams(vmem_limit_bytes=24 << 20),
        **options,
    )


def array(*shape, dtype=jnp.float32):
    return jax.ShapeDtypeStruct(shape, dtype)


def slots(routes, stations, capacity):
    onehot = (routes[:, None] == jnp.arange(stations, dtype=jnp.int32)[None, :]).astype(jnp.int32)
    ranking = jnp.sum((jnp.cumsum(onehot, axis=0) - onehot) * onehot, axis=1)
    return routes * capacity + jnp.minimum(ranking, capacity - 1)


def shards(beam_first, beam_second, green_smooth, green_slope, destination):
    resident = beam_first[0, 0]
    opposing = (beam_second[0, 0],)
    groups = lax.axis_size("dom")
    stations = lax.axis_size("station")
    count = resident.shape[1]
    block_count = count // BLOCK
    capacity = max(2, 2 * block_count // stations)
    scale = STRENGTH * GRID * GRID / (count * groups)
    half, whole = array(2, count), array(4, count)
    density, densities = array(GRID, GRID), array(2, GRID, GRID)
    table = array(2 * GRID, GRID, dtype=jnp.bfloat16)
    place = slots(destination[0, :, 0].astype(jnp.int32), stations, capacity)

    total = local(first_kernel, densities)(resident, opposing[0])
    for front_index in range(FRONTS - 1):
        total = summed(total, "dom")
        positions, moments, other = local(
            functools.partial(opposing_kernel, scale, len(opposing) == 2), (half, half, table)
        )(total, green_smooth, green_slope, *opposing)
        opposing = (shifted(positions, "station", 1), shifted(moments, "station", 1))
        resident, part = local(resident_kernel, (whole, density))(other, resident)
        total = local(arrival_kernel, densities)(opposing[0], part)
    total = summed(total, "dom")
    vmem = pl.BlockSpec(memory_space=pltpu.VMEM)
    outgoing, own = local(
        functools.partial(last_kernel, scale),
        (array(stations * capacity, 4, BLOCK), table),
        in_specs=[pl.BlockSpec(memory_space=pltpu.SMEM)] + [vmem] * 4,
        out_specs=(vmem, vmem),
        scratch_shapes=[pltpu.VMEM((4, count), jnp.float32)],
    )(place, total, green_smooth, green_slope, resident)
    outgoing = outgoing.reshape(stations, capacity, 4, BLOCK)
    arrived = lax.all_to_all(outgoing, "station", split_axis=0, concat_axis=0, tiled=True)
    opposing = local(final_kernel, whole)(own, *opposing)
    return (arrived[None, None], opposing[None, None])


def solution(mesh):
    placed = (
        P("station", "dom", None, None),
        P("station", "dom", None, None),
        P(),
        P(),
        P("station", "dom", None),
    )
    return jax.shard_map(
        shards,
        mesh=mesh,
        in_specs=placed,
        out_specs=(P("station", "dom", None, None, None, None), P("station", "dom", None, None)),
        check_vma=False,
    )
```

```python
import functools

import jax
import jax.numpy as jnp
from jax import lax
from jax.experimental import pallas as pl
from jax.experimental.pallas import tpu as pltpu
from jax.sharding import PartitionSpec as P


GRID = 128
FRONTS = 4
BLOCK = 128
TILE = 4096
ROWS = 16


EDGE = 4.0
DRIFT = 0.05
STRENGTH = 0.06
HIGH = lax.Precision.HIGHEST
SPACING = 2.0 * EDGE / (GRID - 1)


def shifted(value, axis, steps):
    count = lax.axis_size(axis)
    pairs = [(source, (source + steps) % count) for source in range(count)]
    return lax.ppermute(value, axis, pairs)


def summed(value, axis):
    count = lax.axis_size(axis)
    step = 1
    while step < count:
        pairs = [(source, source ^ step) for source in range(count)]
        value = value + lax.ppermute(value.astype(jnp.bfloat16), axis, pairs).astype(jnp.float32)
        step *= 2
    return value


def hat_table(coordinate):
    count = coordinate.shape[1]
    place = jnp.clip((coordinate + EDGE) * (1.0 / SPACING), -2.0, GRID + 2.0)
    cell = jnp.floor(place)
    upper = place - cell
    lower = 1.0 - upper

    def spread(row):
        return jnp.broadcast_to(row, (ROWS, count)).astype(jnp.bfloat16)

    cell, lower, upper = spread(cell), spread(lower), spread(upper)
    none = jnp.zeros((ROWS, count), jnp.bfloat16)
    index = lax.broadcasted_iota(jnp.int32, (ROWS, count), 0).astype(jnp.float32)
    parts = []
    for start in range(0, GRID, ROWS):
        at = (index + float(start)).astype(jnp.bfloat16)
        before = (index + float(start - 1)).astype(jnp.bfloat16)
        parts.append(jnp.where(cell == at, lower, jnp.where(cell == before, upper, none)))
    return jnp.concatenate(parts, axis=0)


def weigh(x, y, hats_ref, tile):
    hats_ref[:GRID, tile] = hat_table(x)
    hats_ref[GRID:, tile] = hat_table(y)
    return lax.dot_general(
        hats_ref[GRID:, tile],
        hats_ref[:GRID, tile],
        (((1,), (1,)), ((), ())),
        preferred_element_type=jnp.float32,
    )


def kick(x, moment_x, y, moment_y, hats_ref, tile, table):
    sampled = jnp.dot(table, hats_ref[:GRID, tile], preferred_element_type=jnp.float32)
    weight_y = hats_ref[GRID:, tile].astype(jnp.float32)
    moment_x = moment_x - jnp.sum(sampled[:GRID] * weight_y, axis=0, keepdims=True)
    moment_y = moment_y - jnp.sum(sampled[GRID:] * weight_y, axis=0, keepdims=True)
    return x + DRIFT * moment_x, moment_x, y + DRIFT * moment_y, moment_y


def tables(density, smooth, slope, scale):
    stacked = density.reshape(2 * GRID, GRID) * scale
    greens = jnp.concatenate([slope, smooth], axis=0)
    inner = lax.dot_general(
        stacked, greens, (((1,), (1,)), ((), ())), precision=HIGH, preferred_element_type=jnp.float32
    )
    by_slope = jnp.concatenate([inner[:GRID, :GRID], inner[GRID:, :GRID]], axis=1)
    by_smooth = jnp.concatenate([inner[:GRID, GRID:], inner[GRID:, GRID:]], axis=1)
    push_x = jnp.dot(smooth, by_slope, precision=HIGH, preferred_element_type=jnp.float32)
    push_y = jnp.dot(slope, by_smooth, precision=HIGH, preferred_element_type=jnp.float32)
    both = jnp.concatenate([push_x, push_y], axis=0).astype(jnp.bfloat16)
    return both[:, :GRID], both[:, GRID:]


def columns(count):
    width = min(TILE, count)
    return [pl.ds(start, width) for start in range(0, count, width)]


def first_kernel(*refs):
    sources, held, (density_ref, *hats), landed = refs[:4], refs[4:8], refs[8:11], refs[11]
    copies = [
        pltpu.make_async_copy(source, place, landed.at[which])
        for which, (source, place) in enumerate(zip(sources, held))
    ]
    for copy in copies:
        copy.start()
    for which in range(2):
        copies[which].wait()
        beam = held[which]
        density_ref[which] = sum(
            weigh(beam[0:1, tile], beam[2:3, tile], hats[which], tile)
            for tile in columns(beam.shape[1])
        )
    for copy in copies[2:]:
        copy.wait()


def rows(sources, tile):
    if len(sources) == 1:
        return [sources[0][row : row + 1, tile] for row in range(4)]
    return [sources[row % 2][row // 2 : row // 2 + 1, tile] for row in range(4)]


def opposing_kernel(scale, density_ref, smooth_ref, slope_ref, hats_ref, *refs):
    own, other = tables(density_ref[...], smooth_ref[...], slope_ref[...], scale)
    *sources, place_ref, moment_ref, table_ref = refs
    table_ref[...] = other
    for tile in columns(place_ref.shape[1]):
        x, moment_x, y, moment_y = kick(*rows(sources, tile), hats_ref, tile, own)
        place_ref[0:1, tile] = x
        place_ref[1:2, tile] = y
        moment_ref[0:1, tile] = moment_x
        moment_ref[1:2, tile] = moment_y


def resident_kernel(table_ref, hats_ref, beam_ref, moved_ref, density_ref, new_hats_ref):
    total = 0.0
    for tile in columns(beam_ref.shape[1]):
        new = kick(*rows([beam_ref], tile), hats_ref, tile, table_ref[...])
        for row in range(4):
            moved_ref[row : row + 1, tile] = new[row]
        total = total + weigh(new[0], new[2], new_hats_ref, tile)
    density_ref[...] = total


def arrival_kernel(place_ref, resident_ref, density_ref, hats_ref):
    density_ref[0] = resident_ref[...]
    density_ref[1] = sum(
        weigh(place_ref[0:1, tile], place_ref[1:2, tile], hats_ref, tile)
        for tile in columns(place_ref.shape[1])
    )


def last_kernel(scale, slots_ref, density_ref, smooth_ref, slope_ref, hats_ref, beam_ref, packed_ref, table_ref, moved_ref):
    table_ref[...], other = tables(density_ref[...], smooth_ref[...], slope_ref[...], scale)
    packed_ref[...] = jnp.zeros_like(packed_ref)
    for tile in columns(beam_ref.shape[1]):
        new = kick(*rows([beam_ref], tile), hats_ref, tile, other)
        for row in range(4):
            moved_ref[row : row + 1, tile] = new[row]
    for block in range(beam_ref.shape[1] // BLOCK):
        packed_ref[slots_ref[block]] = moved_ref[:, block * BLOCK : (block + 1) * BLOCK]


def final_kernel(table_ref, place_ref, moment_ref, out_ref, hats_ref):
    for tile in columns(place_ref.shape[1]):
        hats_ref[:GRID, tile] = hat_table(place_ref[0:1, tile])
        hats_ref[GRID:, tile] = hat_table(place_ref[1:2, tile])
        new = kick(*rows([place_ref, moment_ref], tile), hats_ref, tile, table_ref[...])
        for row in range(4):
            out_ref[row : row + 1, tile] = new[row]


def local(kernel, out_shape, **options):
    return pl.pallas_call(
        kernel,
        out_shape=out_shape,
        compiler_params=pltpu.CompilerParams(vmem_limit_bytes=24 << 20),
        **options,
    )


def array(*shape, dtype=jnp.float32):
    return jax.ShapeDtypeStruct(shape, dtype)


def slots_kernel(capacity, routes_ref, slots_ref, taken_ref):
    for station in range(taken_ref.shape[0]):
        taken_ref[station] = 0

    def place(block, carry):
        station = routes_ref[block]
        taken = taken_ref[station]
        slots_ref[block] = station * capacity + jnp.minimum(taken, capacity - 1)
        taken_ref[station] = taken + 1
        return carry

    lax.fori_loop(0, routes_ref.shape[0], place, 0)


def shards(beam_first, beam_second, green_smooth, green_slope, destination):
    resident = beam_first[0, 0]
    opposing = (beam_second[0, 0],)
    groups = lax.axis_size("dom")
    stations = lax.axis_size("station")
    count = resident.shape[1]
    block_count = count // BLOCK
    capacity = max(2, 2 * block_count // stations)
    scale = STRENGTH * GRID * GRID / (count * groups)
    half, whole = array(2, count), array(4, count)
    density, densities = array(GRID, GRID), array(2, GRID, GRID)
    table = array(2 * GRID, GRID, dtype=jnp.bfloat16)
    hats = array(2 * GRID, count, dtype=jnp.bfloat16)
    vmem, smem = (pl.BlockSpec(memory_space=space) for space in (pltpu.VMEM, pltpu.SMEM))
    place = local(
        functools.partial(slots_kernel, capacity),
        array(block_count, dtype=jnp.int32),
        in_specs=[smem],
        out_specs=smem,
        scratch_shapes=[pltpu.SMEM((stations,), jnp.int32)],
    )(destination[0, :, 0])

    arguments = (resident, opposing[0], green_smooth, green_slope)
    resident, *opposing, smooth, slope, total, resident_hats, opposing_hats = local(
        first_kernel,
        (whole, whole, density, density, densities, hats, hats),
        in_specs=[pl.BlockSpec(memory_space=pltpu.HBM)] * 4,
        out_specs=(vmem,) * 7,
        scratch_shapes=[pltpu.SemaphoreType.DMA((4,))],
    )(*(pltpu.with_memory_space_constraint(value, pltpu.HBM) for value in arguments))
    for front_index in range(FRONTS - 1):
        total = summed(total, "dom")
        positions, moments, other = local(
            functools.partial(opposing_kernel, scale), (half, half, table)
        )(total, smooth, slope, opposing_hats, *opposing)
        positions = shifted(positions, "station", 1)
        moments = shifted(moments, "station", 1)
        opposing = (positions, moments)
        resident, part, resident_hats = local(resident_kernel, (whole, density, hats))(
            other, resident_hats, resident
        )
        last = front_index + 2 == FRONTS
        total, *kept = local(
            arrival_kernel,
            (densities,) if last else (densities, hats),
            scratch_shapes=[pltpu.VMEM(hats.shape, hats.dtype)] if last else [],
        )(positions, part)
        opposing_hats = None if last else kept[0]
    total = summed(total, "dom")
    outgoing, own = local(
        functools.partial(last_kernel, scale),
        (array(stations * capacity, 4, BLOCK), table),
        in_specs=[smem] + [vmem] * 5,
        out_specs=(vmem, vmem),
        scratch_shapes=[pltpu.VMEM((4, count), jnp.float32)],
    )(place, total, smooth, slope, resident_hats, resident)
    outgoing = outgoing.reshape(stations, capacity, 4, BLOCK)
    arrived = lax.all_to_all(outgoing, "station", split_axis=0, concat_axis=0, tiled=True)
    opposing = local(final_kernel, whole, scratch_shapes=[pltpu.VMEM(hats.shape, hats.dtype)])(own, *opposing)
    return (arrived[None, None], opposing[None, None])


def solution(mesh):
    placed = (
        P("station", "dom", None, None),
        P("station", "dom", None, None),
        P(),
        P(),
        P("station", "dom", None),
    )
    return jax.shard_map(
        shards,
        mesh=mesh,
        in_specs=placed,
        out_specs=(P("station", "dom", None, None, None, None), P("station", "dom", None, None)),
        check_vma=False,
    )
```

```python
import functools

import jax
import jax.numpy as jnp
from jax import lax
from jax.experimental import pallas as pl
from jax.experimental.pallas import tpu as pltpu
from jax.sharding import PartitionSpec as P


GRID = 128
FRONTS = 4
BLOCK = 128
TILE = 2048
LINES = 8


EDGE = 4.0
DRIFT = 0.05
STRENGTH = 0.06
HIGH = lax.Precision.HIGHEST
SPACING = 2.0 * EDGE / (GRID - 1)


def shifted(value, axis, steps):
    count = lax.axis_size(axis)
    pairs = [(source, (source + steps) % count) for source in range(count)]
    return lax.ppermute(value, axis, pairs)


def summed(value, axis):
    count = lax.axis_size(axis)
    step = 1
    while step < count:
        pairs = [(source, source ^ step) for source in range(count)]
        other = lax.ppermute(value.astype(jnp.bfloat16), axis, pairs)
        value = value + other.astype(jnp.float32)
        step *= 2
    return value


def cells(coordinate):
    place = jnp.clip((coordinate + EDGE) * (1.0 / SPACING), -2.0, GRID + 2.0)
    cell = jnp.floor(place)
    upper = place - cell
    lower = 1.0 - upper
    odd = jnp.floor(cell * 0.5)
    even = cell - odd
    is_even = even == odd
    return (even, jnp.where(is_even, lower, upper)), (odd, jnp.where(is_even, upper, lower))


def hat_table(coordinate):
    count = coordinate.shape[1]
    none = jnp.zeros((2 * LINES, count), jnp.bfloat16)
    index = lax.broadcasted_iota(jnp.int32, none.shape, 0).astype(jnp.float32)
    parts = []
    for pair in cells(coordinate):
        cell, weight = (jnp.concatenate([row, row], axis=0).astype(jnp.bfloat16) for row in pair)
        for start in range(0, GRID // 2, 2 * LINES):
            at = (index + float(start)).astype(jnp.bfloat16)
            parts.append(jnp.where(cell == at, weight, none))
    return jnp.concatenate(parts, axis=0)


def deposit(x, y):
    return lax.dot_general(
        hat_table(y), hat_table(x), (((1,), (1,)), ((), ())), preferred_element_type=jnp.float32
    )


def kick(x, moment_x, y, moment_y, table):
    sampled = jnp.dot(table, hat_table(x), preferred_element_type=jnp.float32)
    index = lax.broadcasted_iota(jnp.int32, x.shape, 0).astype(jnp.float32)
    moments = [moment_x, moment_y]
    pushes = [0.0, 0.0]
    block = 0
    for cell, weight in cells(y):
        weight = weight.astype(jnp.bfloat16).astype(jnp.float32)
        found = [jnp.zeros(x.shape, jnp.float32)] * 2
        for start in range(0, GRID // 2, LINES):
            here = cell == index + float(start)
            for which in range(2):
                part = sampled[block * LINES : (block + 1) * LINES]
                found[which] = jnp.where(here, part, found[which])
                block += 1
        pushes = [push + weight * part for push, part in zip(pushes, found)]
    for which, push in enumerate(pushes):
        shift = LINES // 2
        while shift:
            push = push + pltpu.roll(push, shift, 0)
            shift //= 2
        moments[which] = moments[which] - push
    moment_x, moment_y = moments
    return x + DRIFT * moment_x, moment_x, y + DRIFT * moment_y, moment_y


def halves(value):
    high = value.astype(jnp.bfloat16)
    return high, (value - high.astype(jnp.float32)).astype(jnp.bfloat16)


def tables(density, smooth, slope, scale):
    high, low = halves(density.reshape(2 * GRID, GRID) * scale)
    left = jnp.concatenate([high, low, high], axis=1)
    inner = lax.dot_general(
        left,
        jnp.concatenate([slope, smooth], axis=0),
        (((1,), (1,)), ((), ())),
        preferred_element_type=jnp.float32,
    )
    pushes = []
    for which, green in enumerate((smooth, slope)):
        part = inner[:, which * GRID : (which + 1) * GRID]
        high, low = halves(jnp.concatenate([part[:GRID], part[GRID:]], axis=1))
        right = jnp.concatenate([high, low, high], axis=0)
        pushes.append(jnp.dot(green, right, preferred_element_type=jnp.float32))
    both = jnp.concatenate(
        [push[start : start + LINES] for start in range(0, GRID, LINES) for push in pushes], axis=0
    ).astype(jnp.bfloat16)
    return both[:, :GRID], both[:, GRID:]


def greens_kernel(smooth_ref, slope_ref, *outs):
    row = lax.broadcasted_iota(jnp.int32, (GRID, GRID), 0)
    column = lax.broadcasted_iota(jnp.int32, (GRID, GRID), 1)
    chosen = jnp.where(row < GRID // 2, 2 * row, 2 * row - (GRID - 1))
    order = (column == chosen).astype(jnp.float32)
    for ref, out_ref in zip((smooth_ref, slope_ref), outs):
        moved = jnp.dot(order, ref[...], precision=HIGH, preferred_element_type=jnp.float32)
        moved = lax.dot_general(
            moved, order, (((1,), (1,)), ((), ())), precision=HIGH, preferred_element_type=jnp.float32
        )
        high, low = halves(moved)
        for place, part in enumerate((high, high, low)):
            out_ref[:, place * GRID : (place + 1) * GRID] = part


def columns(count):
    width = min(TILE, count)
    return [pl.ds(start, width) for start in range(0, count, width)]


def first_kernel(resident_hbm, opposing_hbm, resident_ref, opposing_ref, density_ref, landed):
    held = (resident_ref, opposing_ref)
    copies = [
        pltpu.make_async_copy(source, place, landed.at[which])
        for which, (source, place) in enumerate(zip((resident_hbm, opposing_hbm), held))
    ]
    for copy in copies:
        copy.start()
    for which, copy in enumerate(copies):
        copy.wait()
        beam = held[which]
        density_ref[which] = sum(
            deposit(line(beam, 0, tile), line(beam, 2, tile)) for tile in columns(beam.shape[1])
        )


def line(ref, row, tile):
    return jnp.broadcast_to(ref[row : row + 1, tile], (LINES, tile.size))


def rows(sources, tile):
    if len(sources) == 1:
        return [line(sources[0], row, tile) for row in range(4)]
    return [line(sources[row % 2], row // 2, tile) for row in range(4)]


def opposing_kernel(scale, density_ref, smooth_ref, slope_ref, *refs):
    own, other = tables(density_ref[...], smooth_ref[...], slope_ref[...], scale)
    *sources, place_ref, moment_ref, table_ref = refs
    table_ref[...] = other
    for tile in columns(place_ref.shape[1]):
        x, moment_x, y, moment_y = kick(*rows(sources, tile), own)
        place_ref[0:1, tile] = x[:1]
        place_ref[1:2, tile] = y[:1]
        moment_ref[0:1, tile] = moment_x[:1]
        moment_ref[1:2, tile] = moment_y[:1]


def resident_kernel(table_ref, beam_ref, moved_ref, density_ref):
    total = 0.0
    for tile in columns(beam_ref.shape[1]):
        new = kick(*rows([beam_ref], tile), table_ref[...])
        for row in range(4):
            moved_ref[row : row + 1, tile] = new[row][:1]
        total = total + deposit(new[0], new[2])
    density_ref[...] = total


def arrival_kernel(place_ref, resident_ref, density_ref):
    density_ref[0] = resident_ref[...]
    density_ref[1] = sum(
        deposit(line(place_ref, 0, tile), line(place_ref, 1, tile)) for tile in columns(place_ref.shape[1])
    )


def last_kernel(scale, slots_ref, density_ref, smooth_ref, slope_ref, beam_ref, packed_ref, table_ref, moved_ref):
    table_ref[...], other = tables(density_ref[...], smooth_ref[...], slope_ref[...], scale)
    packed_ref[...] = jnp.zeros_like(packed_ref)
    for tile in columns(beam_ref.shape[1]):
        new = kick(*rows([beam_ref], tile), other)
        for row in range(4):
            moved_ref[row : row + 1, tile] = new[row][:1]
    for block in range(beam_ref.shape[1] // BLOCK):
        packed_ref[slots_ref[block]] = moved_ref[:, block * BLOCK : (block + 1) * BLOCK]


def final_kernel(table_ref, place_ref, moment_ref, out_ref):
    for tile in columns(place_ref.shape[1]):
        new = kick(*rows([place_ref, moment_ref], tile), table_ref[...])
        for row in range(4):
            out_ref[row : row + 1, tile] = new[row][:1]


def local(kernel, out_shape, **options):
    return pl.pallas_call(
        kernel,
        out_shape=out_shape,
        compiler_params=pltpu.CompilerParams(vmem_limit_bytes=24 << 20),
        **options,
    )


def array(*shape, dtype=jnp.float32):
    return jax.ShapeDtypeStruct(shape, dtype)


def slots_kernel(capacity, routes_ref, slots_ref, taken_ref):
    for station in range(taken_ref.shape[0]):
        taken_ref[station] = 0

    def place(block, carry):
        station = routes_ref[block]
        taken = taken_ref[station]
        slots_ref[block] = station * capacity + jnp.minimum(taken, capacity - 1)
        taken_ref[station] = taken + 1
        return carry

    lax.fori_loop(0, routes_ref.shape[0], place, 0)


def shards(beam_first, beam_second, green_smooth, green_slope, destination):
    resident = beam_first[0, 0]
    opposing = (beam_second[0, 0],)
    groups = lax.axis_size("dom")
    stations = lax.axis_size("station")
    count = resident.shape[1]
    block_count = count // BLOCK
    capacity = max(2, 2 * block_count // stations)
    scale = STRENGTH * GRID * GRID / (count * groups)
    half, whole = array(2, count), array(4, count)
    density, densities = array(GRID, GRID), array(2, GRID, GRID)
    table = array(2 * GRID, GRID, dtype=jnp.bfloat16)
    vmem, smem = (pl.BlockSpec(memory_space=space) for space in (pltpu.VMEM, pltpu.SMEM))
    place = local(
        functools.partial(slots_kernel, capacity),
        array(block_count, dtype=jnp.int32),
        in_specs=[smem],
        out_specs=smem,
        scratch_shapes=[pltpu.SMEM((stations,), jnp.int32)],
    )(destination[0, :, 0])

    resident, *opposing, total = local(
        first_kernel,
        (whole, whole, densities),
        in_specs=[pl.BlockSpec(memory_space=pltpu.HBM)] * 2,
        out_specs=(vmem,) * 3,
        scratch_shapes=[pltpu.SemaphoreType.DMA((2,))],
    )(*(pltpu.with_memory_space_constraint(value, pltpu.HBM) for value in (resident, opposing[0])))
    wide = array(GRID, 3 * GRID, dtype=jnp.bfloat16)
    smooth, slope = local(greens_kernel, (wide, wide))(green_smooth, green_slope)
    total = summed(total, "dom")
    for _ in range(FRONTS - 1):
        positions, moments, other = local(
            functools.partial(opposing_kernel, scale), (half, half, table)
        )(total, smooth, slope, *opposing)
        positions = shifted(positions, "station", 1)
        moments = shifted(moments, "station", 1)
        opposing = (positions, moments)
        resident, part = local(resident_kernel, (whole, density))(other, resident)
        total = local(arrival_kernel, densities)(positions, part)
        total = summed(total, "dom")
    outgoing, own = local(
        functools.partial(last_kernel, scale),
        (array(stations * capacity, 4, BLOCK), table),
        in_specs=[smem] + [vmem] * 4,
        out_specs=(vmem, vmem),
        scratch_shapes=[pltpu.VMEM((4, count), jnp.float32)],
    )(place, total, smooth, slope, resident)
    outgoing = outgoing.reshape(stations, capacity, 4, BLOCK)
    arrived = lax.all_to_all(outgoing, "station", split_axis=0, concat_axis=0, tiled=True)
    opposing = local(final_kernel, whole)(own, *opposing)
    return (arrived[None, None], opposing[None, None])


def solution(mesh):
    placed = (
        P("station", "dom", None, None),
        P("station", "dom", None, None),
        P(),
        P(),
        P("station", "dom", None),
    )
    return jax.shard_map(
        shards,
        mesh=mesh,
        in_specs=placed,
        out_specs=(P("station", "dom", None, None, None, None), P("station", "dom", None, None)),
        check_vma=False,
    )
```

```python
import functools

import jax
import jax.numpy as jnp
from jax import lax
from jax.experimental import pallas as pl
from jax.experimental.pallas import tpu as pltpu
from jax.sharding import PartitionSpec as P


GRID = 128
FRONTS = 4
BLOCK = 128
TILE = 2048
LINES = 8


EDGE = 4.0
DRIFT = 0.05
STRENGTH = 0.06
HIGH = lax.Precision.HIGHEST
SPACING = 2.0 * EDGE / (GRID - 1)


def shifted(value, axis, steps):
    count = lax.axis_size(axis)
    pairs = [(source, (source + steps) % count) for source in range(count)]
    return lax.ppermute(value, axis, pairs)


def summed(value, axis):
    count = lax.axis_size(axis)
    step = 1
    while step < count:
        pairs = [(source, source ^ step) for source in range(count)]
        other = lax.ppermute(value.astype(jnp.bfloat16), axis, pairs)
        value = value + other.astype(jnp.float32)
        step *= 2
    return value


def cells(coordinate):
    place = jnp.clip((coordinate + EDGE) * (1.0 / SPACING), -2.0, GRID + 2.0)
    cell = jnp.floor(place)
    upper = place - cell
    lower = 1.0 - upper
    odd = jnp.floor(cell * 0.5)
    even = cell - odd
    is_even = even == odd
    return (even, jnp.where(is_even, lower, upper)), (odd, jnp.where(is_even, upper, lower))


def hat_table(coordinate):
    count = coordinate.shape[1]
    none = jnp.zeros((2 * LINES, count), jnp.bfloat16)
    index = lax.broadcasted_iota(jnp.int32, none.shape, 0).astype(jnp.float32)
    parts = []
    for pair in cells(coordinate):
        cell, weight = (jnp.concatenate([row, row], axis=0).astype(jnp.bfloat16) for row in pair)
        for start in range(0, GRID // 2, 2 * LINES):
            at = (index + float(start)).astype(jnp.bfloat16)
            parts.append(jnp.where(cell == at, weight, none))
    return jnp.concatenate(parts, axis=0)


def deposit(x, y):
    return lax.dot_general(
        hat_table(y), hat_table(x), (((1,), (1,)), ((), ())), preferred_element_type=jnp.float32
    )


def kick(x, moment_x, y, moment_y, table):
    sampled = jnp.dot(table, hat_table(x), preferred_element_type=jnp.float32)
    index = lax.broadcasted_iota(jnp.int32, x.shape, 0).astype(jnp.float32)
    moments = [moment_x, moment_y]
    pushes = [0.0, 0.0]
    block = 0
    for cell, weight in cells(y):
        weight = weight.astype(jnp.bfloat16).astype(jnp.float32)
        found = [jnp.zeros(x.shape, jnp.float32)] * 2
        for start in range(0, GRID // 2, LINES):
            here = cell == index + float(start)
            for which in range(2):
                part = sampled[block * LINES : (block + 1) * LINES]
                found[which] = jnp.where(here, part, found[which])
                block += 1
        pushes = [push + weight * part for push, part in zip(pushes, found)]
    for which, push in enumerate(pushes):
        shift = LINES // 2
        while shift:
            push = push + pltpu.roll(push, shift, 0)
            shift //= 2
        moments[which] = moments[which] - push
    moment_x, moment_y = moments
    return x + DRIFT * moment_x, moment_x, y + DRIFT * moment_y, moment_y


def halves(value):
    high = value.astype(jnp.bfloat16)
    return high, (value - high.astype(jnp.float32)).astype(jnp.bfloat16)


def table_of(density, smooth, slope, scale):
    high, low = halves(density * scale)
    inner = lax.dot_general(
        jnp.concatenate([high, low, high], axis=1),
        jnp.concatenate([slope, smooth], axis=0),
        (((1,), (1,)), ((), ())),
        preferred_element_type=jnp.float32,
    )
    pushes = []
    for which, green in enumerate((smooth, slope)):
        high, low = halves(inner[:, which * GRID : (which + 1) * GRID])
        right = jnp.concatenate([high, low, high], axis=0)
        pushes.append(jnp.dot(green, right, preferred_element_type=jnp.float32))
    return jnp.concatenate(
        [push[start : start + LINES] for start in range(0, GRID, LINES) for push in pushes], axis=0
    ).astype(jnp.bfloat16)


def greens_kernel(smooth_ref, slope_ref, *outs):
    row = lax.broadcasted_iota(jnp.int32, (GRID, GRID), 0)
    column = lax.broadcasted_iota(jnp.int32, (GRID, GRID), 1)
    chosen = jnp.where(row < GRID // 2, 2 * row, 2 * row - (GRID - 1))
    order = (column == chosen).astype(jnp.float32)
    for ref, out_ref in zip((smooth_ref, slope_ref), outs):
        moved = jnp.dot(order, ref[...], precision=HIGH, preferred_element_type=jnp.float32)
        moved = lax.dot_general(
            moved, order, (((1,), (1,)), ((), ())), precision=HIGH, preferred_element_type=jnp.float32
        )
        high, low = halves(moved)
        for place, part in enumerate((high, high, low)):
            out_ref[:, place * GRID : (place + 1) * GRID] = part


def columns(count):
    width = min(TILE, count)
    return [pl.ds(start, width) for start in range(0, count, width)]


def first_kernel(resident_hbm, opposing_hbm, resident_ref, opposing_ref, density_ref, landed):
    held = (resident_ref, opposing_ref)
    copies = [
        pltpu.make_async_copy(source, place, landed.at[which])
        for which, (source, place) in enumerate(zip((resident_hbm, opposing_hbm), held))
    ]
    for copy in copies:
        copy.start()
    for which, copy in enumerate(copies):
        copy.wait()
        beam = held[which]
        density_ref[which] = sum(
            deposit(line(beam, 0, tile), line(beam, 2, tile)) for tile in columns(beam.shape[1])
        )


def line(ref, row, tile):
    return jnp.broadcast_to(ref[row : row + 1, tile], (LINES, tile.size))


def rows(sources, tile):
    if len(sources) == 1:
        return [line(sources[0], row, tile) for row in range(4)]
    return [line(sources[row % 2], row // 2, tile) for row in range(4)]


def opposing_kernel(scale, density_ref, smooth_ref, slope_ref, *refs):
    table = table_of(density_ref[0], smooth_ref[...], slope_ref[...], scale)
    *sources, place_ref, moment_ref = refs
    for tile in columns(place_ref.shape[1]):
        x, moment_x, y, moment_y = kick(*rows(sources, tile), table)
        place_ref[0:1, tile] = x[:1]
        place_ref[1:2, tile] = y[:1]
        moment_ref[0:1, tile] = moment_x[:1]
        moment_ref[1:2, tile] = moment_y[:1]


def resident_kernel(scale, density_ref, smooth_ref, slope_ref, beam_ref, moved_ref, part_ref):
    table = table_of(density_ref[1], smooth_ref[...], slope_ref[...], scale)
    total = 0.0
    for tile in columns(beam_ref.shape[1]):
        new = kick(*rows([beam_ref], tile), table)
        for row in range(4):
            moved_ref[row : row + 1, tile] = new[row][:1]
        total = total + deposit(new[0], new[2])
    part_ref[...] = total


def arrival_kernel(place_ref, resident_ref, density_ref):
    density_ref[0] = resident_ref[...]
    density_ref[1] = sum(
        deposit(line(place_ref, 0, tile), line(place_ref, 1, tile)) for tile in columns(place_ref.shape[1])
    )


def last_kernel(scale, slots_ref, density_ref, smooth_ref, slope_ref, beam_ref, *refs):
    *packed, moved_ref, slots_out = refs
    table = table_of(density_ref[1], smooth_ref[...], slope_ref[...], scale)
    slots_out[...] = jnp.zeros_like(slots_out)
    for tile in columns(beam_ref.shape[1]):
        new = kick(*rows([beam_ref], tile), table)
        for row in range(4):
            moved_ref[row : row + 1, tile] = new[row][:1]
    for block in range(beam_ref.shape[1] // BLOCK):
        slots_out[slots_ref[block]] = moved_ref[:, block * BLOCK : (block + 1) * BLOCK]
    for distance, ref in enumerate(packed):
        capacity = ref.shape[0]
        ref[...] = slots_out[distance * capacity : (distance + 1) * capacity]


def final_kernel(scale, density_ref, smooth_ref, slope_ref, place_ref, moment_ref, out_ref):
    table = table_of(density_ref[0], smooth_ref[...], slope_ref[...], scale)
    for tile in columns(place_ref.shape[1]):
        new = kick(*rows([place_ref, moment_ref], tile), table)
        for row in range(4):
            out_ref[row : row + 1, tile] = new[row][:1]


def gather_kernel(me_ref, *refs):
    *parts, out_hbm, landed = refs
    copies = [
        pltpu.make_async_copy(part, out_hbm.at[me_ref[0] ^ distance], landed.at[distance])
        for distance, part in enumerate(parts)
    ]
    for copy in copies:
        copy.start()
    for copy in copies:
        copy.wait()


def local(kernel, out_shape, **options):
    return pl.pallas_call(
        kernel,
        out_shape=out_shape,
        compiler_params=pltpu.CompilerParams(vmem_limit_bytes=24 << 20),
        **options,
    )


def array(*shape, dtype=jnp.float32):
    return jax.ShapeDtypeStruct(shape, dtype)


def slots_kernel(capacity, me_ref, routes_ref, slots_ref, taken_ref):
    for station in range(taken_ref.shape[0]):
        taken_ref[station] = 0

    def place(block, carry):
        distance = routes_ref[block] ^ me_ref[0]
        taken = taken_ref[distance]
        slots_ref[block] = distance * capacity + jnp.minimum(taken, capacity - 1)
        taken_ref[distance] = taken + 1
        return carry

    lax.fori_loop(0, routes_ref.shape[0], place, 0)


def shards(beam_first, beam_second, green_smooth, green_slope, destination):
    resident = beam_first[0, 0]
    opposing = (beam_second[0, 0],)
    groups = lax.axis_size("dom")
    stations = lax.axis_size("station")
    count = resident.shape[1]
    block_count = count // BLOCK
    capacity = max(2, 2 * block_count // stations)
    scale = STRENGTH * GRID * GRID / (count * groups)
    half, whole = array(2, count), array(4, count)
    density, densities = array(GRID, GRID), array(2, GRID, GRID)
    me = jnp.full((1,), lax.axis_index("station"), jnp.int32)
    vmem, smem = (pl.BlockSpec(memory_space=space) for space in (pltpu.VMEM, pltpu.SMEM))
    place = local(
        functools.partial(slots_kernel, capacity),
        array(block_count, dtype=jnp.int32),
        in_specs=[smem] * 2,
        out_specs=smem,
        scratch_shapes=[pltpu.SMEM((stations,), jnp.int32)],
    )(me, destination[0, :, 0])

    resident, *opposing, total = local(
        first_kernel,
        (whole, whole, densities),
        in_specs=[pl.BlockSpec(memory_space=pltpu.HBM)] * 2,
        out_specs=(vmem,) * 3,
        scratch_shapes=[pltpu.SemaphoreType.DMA((2,))],
    )(*(pltpu.with_memory_space_constraint(value, pltpu.HBM) for value in (resident, opposing[0])))
    wide = array(GRID, 3 * GRID, dtype=jnp.bfloat16)
    smooth, slope = local(greens_kernel, (wide, wide))(green_smooth, green_slope)
    total = summed(total, "dom")
    for _ in range(FRONTS - 1):
        positions, moments = local(functools.partial(opposing_kernel, scale), (half, half))(
            total, smooth, slope, *opposing
        )
        positions = shifted(positions, "station", 1)
        moments = shifted(moments, "station", 1)
        opposing = (positions, moments)
        resident, part = local(
            functools.partial(resident_kernel, scale), (whole, density)
        )(total, smooth, slope, resident)
        total = local(arrival_kernel, densities)(positions, part)
        total = summed(total, "dom")
    blocks = array(capacity, 4, BLOCK)
    parts = local(
        functools.partial(last_kernel, scale),
        (blocks,) * stations,
        in_specs=[smem] + [vmem] * 4,
        out_specs=(vmem,) * stations,
        scratch_shapes=[
            pltpu.VMEM((4, count), jnp.float32),
            pltpu.VMEM((stations * capacity, 4, BLOCK), jnp.float32),
        ],
    )(place, total, smooth, slope, resident)
    parts = [
        lax.ppermute(part, "station", [(source, source ^ distance) for source in range(stations)])
        if distance
        else part
        for distance, part in enumerate(parts)
    ]
    opposing = local(functools.partial(final_kernel, scale), whole)(total, smooth, slope, *opposing)
    arrived = local(
        gather_kernel,
        array(stations, capacity, 4, BLOCK),
        in_specs=[smem] + [vmem] * stations,
        out_specs=pl.BlockSpec(memory_space=pltpu.HBM),
        scratch_shapes=[pltpu.SemaphoreType.DMA((stations,))],
    )(me, *parts)
    return (arrived[None, None], opposing[None, None])


def solution(mesh):
    placed = (
        P("station", "dom", None, None),
        P("station", "dom", None, None),
        P(),
        P(),
        P("station", "dom", None),
    )
    return jax.shard_map(
        shards,
        mesh=mesh,
        in_specs=placed,
        out_specs=(P("station", "dom", None, None, None, None), P("station", "dom", None, None)),
        check_vma=False,
    )
```

```python
import functools

import jax
import jax.numpy as jnp
from jax import lax
from jax.experimental import pallas as pl
from jax.experimental.pallas import tpu as pltpu
from jax.sharding import PartitionSpec as P


GRID = 128
FRONTS = 4
BLOCK = 128
TILE = 2048
LINES = 8


EDGE = 4.0
DRIFT = 0.05
STRENGTH = 0.06
HIGH = lax.Precision.HIGHEST
SPACING = 2.0 * EDGE / (GRID - 1)


def shifted(value, axis, steps):
    count = lax.axis_size(axis)
    pairs = [(source, (source + steps) % count) for source in range(count)]
    return lax.ppermute(value, axis, pairs)


def paired(value, axis, distance):
    pairs = [(source, source ^ distance) for source in range(lax.axis_size(axis))]
    return lax.ppermute(value, axis, pairs)


def summed(kept, sent, axis):
    value = kept + paired(sent, axis, 1).astype(jnp.float32)
    sent = value.astype(jnp.bfloat16)
    far = [paired(sent, axis, distance) for distance in range(2, lax.axis_size(axis), 2)]
    return value + sum(part.astype(jnp.float32) for part in reversed(far))


def cells(coordinate):
    place = jnp.clip((coordinate + EDGE) * (1.0 / SPACING), -2.0, GRID + 2.0)
    cell = jnp.floor(place)
    upper = place - cell
    lower = 1.0 - upper
    odd = jnp.floor(cell * 0.5)
    even = cell - odd
    is_even = even == odd
    return (even, jnp.where(is_even, lower, upper)), (odd, jnp.where(is_even, upper, lower))


def hat_table(coordinate):
    count = coordinate.shape[1]
    none = jnp.zeros((2 * LINES, count), jnp.bfloat16)
    index = lax.broadcasted_iota(jnp.int32, none.shape, 0).astype(jnp.float32)
    parts = []
    for pair in cells(coordinate):
        cell, weight = (jnp.concatenate([row, row], axis=0).astype(jnp.bfloat16) for row in pair)
        for start in range(0, GRID // 2, 2 * LINES):
            at = (index + float(start)).astype(jnp.bfloat16)
            parts.append(jnp.where(cell == at, weight, none))
    return jnp.concatenate(parts, axis=0)


def deposit(x, y):
    return lax.dot_general(
        hat_table(y), hat_table(x), (((1,), (1,)), ((), ())), preferred_element_type=jnp.float32
    )


def kick(x, moment_x, y, moment_y, table):
    sampled = jnp.dot(table, hat_table(x), preferred_element_type=jnp.float32)
    index = lax.broadcasted_iota(jnp.int32, x.shape, 0).astype(jnp.float32)
    moments = [moment_x, moment_y]
    pushes = [0.0, 0.0]
    block = 0
    for cell, weight in cells(y):
        weight = weight.astype(jnp.bfloat16).astype(jnp.float32)
        found = [jnp.zeros(x.shape, jnp.float32)] * 2
        for start in range(0, GRID // 2, LINES):
            here = cell == index + float(start)
            for which in range(2):
                part = sampled[block * LINES : (block + 1) * LINES]
                found[which] = jnp.where(here, part, found[which])
                block += 1
        pushes = [push + weight * part for push, part in zip(pushes, found)]
    for which, push in enumerate(pushes):
        shift = LINES // 2
        while shift:
            push = push + pltpu.roll(push, shift, 0)
            shift //= 2
        moments[which] = moments[which] - push
    moment_x, moment_y = moments
    return x + DRIFT * moment_x, moment_x, y + DRIFT * moment_y, moment_y


def halves(value):
    high = value.astype(jnp.bfloat16)
    return high, (value - high.astype(jnp.float32)).astype(jnp.bfloat16)


def table_of(density, smooth, slope, scale):
    high, low = halves(density * scale)
    inner = lax.dot_general(
        jnp.concatenate([high, low, high], axis=1),
        jnp.concatenate([slope, smooth], axis=0),
        (((1,), (1,)), ((), ())),
        preferred_element_type=jnp.float32,
    )
    pushes = []
    for which, green in enumerate((smooth, slope)):
        high, low = halves(inner[:, which * GRID : (which + 1) * GRID])
        right = jnp.concatenate([high, low, high], axis=0)
        pushes.append(jnp.dot(green, right, preferred_element_type=jnp.float32))
    return jnp.concatenate(
        [push[start : start + LINES] for start in range(0, GRID, LINES) for push in pushes], axis=0
    ).astype(jnp.bfloat16)


def greens_kernel(smooth_ref, slope_ref, *outs):
    row = lax.broadcasted_iota(jnp.int32, (GRID, GRID), 0)
    column = lax.broadcasted_iota(jnp.int32, (GRID, GRID), 1)
    chosen = jnp.where(row < GRID // 2, 2 * row, 2 * row - (GRID - 1))
    order = (column == chosen).astype(jnp.float32)
    for ref, out_ref in zip((smooth_ref, slope_ref), outs):
        moved = jnp.dot(order, ref[...], precision=HIGH, preferred_element_type=jnp.float32)
        moved = lax.dot_general(
            moved, order, (((1,), (1,)), ((), ())), precision=HIGH, preferred_element_type=jnp.float32
        )
        high, low = halves(moved)
        for place, part in enumerate((high, high, low)):
            out_ref[:, place * GRID : (place + 1) * GRID] = part


def columns(count):
    width = min(TILE, count)
    return [pl.ds(start, width) for start in range(0, count, width)]


def share(resident, opposing, kept_ref, sent_ref):
    even = lax.rem(lax.axis_index("dom"), 2) == 0
    kept_ref[...] = jnp.where(even, resident, opposing)
    sent_ref[...] = jnp.where(even, opposing, resident).astype(jnp.bfloat16)


def chosen(which, own_ref, other_ref):
    own = lax.rem(lax.axis_index("dom"), 2) == which
    return jnp.where(own, own_ref[...], other_ref[...])


def first_kernel(resident_hbm, opposing_hbm, resident_ref, opposing_ref, kept_ref, sent_ref, landed):
    held = (resident_ref, opposing_ref)
    copies = [
        pltpu.make_async_copy(source, place, landed.at[which])
        for which, (source, place) in enumerate(zip((resident_hbm, opposing_hbm), held))
    ]
    for copy in copies:
        copy.start()
    densities = []
    for copy in copies:
        copy.wait()
    for beam in held:
        densities.append(
            sum(deposit(line(beam, 0, tile), line(beam, 2, tile)) for tile in columns(beam.shape[1]))
        )
    share(*densities, kept_ref, sent_ref)


def line(ref, row, tile):
    return jnp.broadcast_to(ref[row : row + 1, tile], (LINES, tile.size))


def rows(sources, tile):
    if len(sources) == 1:
        return [line(sources[0], row, tile) for row in range(4)]
    return [line(sources[row % 2], row // 2, tile) for row in range(4)]


def table_kernel(scale, density_ref, smooth_ref, slope_ref, table_ref):
    table_ref[...] = table_of(density_ref[...], smooth_ref[...], slope_ref[...], scale)


def opposing_kernel(own_ref, other_ref, *refs):
    table = chosen(0, own_ref, other_ref)
    *sources, place_ref, moment_ref = refs
    for tile in columns(place_ref.shape[1]):
        x, moment_x, y, moment_y = kick(*rows(sources, tile), table)
        place_ref[0:1, tile] = x[:1]
        place_ref[1:2, tile] = y[:1]
        moment_ref[0:1, tile] = moment_x[:1]
        moment_ref[1:2, tile] = moment_y[:1]


def resident_kernel(own_ref, other_ref, beam_ref, moved_ref, part_ref):
    table = chosen(1, own_ref, other_ref)
    total = 0.0
    for tile in columns(beam_ref.shape[1]):
        new = kick(*rows([beam_ref], tile), table)
        for row in range(4):
            moved_ref[row : row + 1, tile] = new[row][:1]
        total = total + deposit(new[0], new[2])
    part_ref[...] = total


def arrival_kernel(place_ref, resident_ref, kept_ref, sent_ref):
    total = sum(
        deposit(line(place_ref, 0, tile), line(place_ref, 1, tile)) for tile in columns(place_ref.shape[1])
    )
    share(resident_ref[...], total, kept_ref, sent_ref)


def last_kernel(slots_ref, own_ref, other_ref, beam_ref, *refs):
    *packed, moved_ref, slots_out = refs
    table = chosen(1, own_ref, other_ref)
    slots_out[...] = jnp.zeros_like(slots_out)
    for tile in columns(beam_ref.shape[1]):
        new = kick(*rows([beam_ref], tile), table)
        for row in range(4):
            moved_ref[row : row + 1, tile] = new[row][:1]
    for block in range(beam_ref.shape[1] // BLOCK):
        slots_out[slots_ref[block]] = moved_ref[:, block * BLOCK : (block + 1) * BLOCK]
    for distance, ref in enumerate(packed):
        capacity = ref.shape[0]
        ref[...] = slots_out[distance * capacity : (distance + 1) * capacity]


def final_kernel(own_ref, other_ref, place_ref, moment_ref, out_ref):
    table = chosen(0, own_ref, other_ref)
    for tile in columns(place_ref.shape[1]):
        new = kick(*rows([place_ref, moment_ref], tile), table)
        for row in range(4):
            out_ref[row : row + 1, tile] = new[row][:1]


def gather_kernel(*refs):
    *parts, out_hbm, landed = refs
    me = lax.axis_index("station")
    copies = [
        pltpu.make_async_copy(part, out_hbm.at[me ^ distance], landed.at[distance])
        for distance, part in enumerate(parts)
    ]
    for copy in copies:
        copy.start()
    for copy in copies:
        copy.wait()


def local(kernel, out_shape, **options):
    return pl.pallas_call(
        kernel,
        out_shape=out_shape,
        compiler_params=pltpu.CompilerParams(vmem_limit_bytes=24 << 20),
        **options,
    )


def array(*shape, dtype=jnp.float32):
    return jax.ShapeDtypeStruct(shape, dtype)


def slots_kernel(capacity, routes_ref, slots_ref, taken_ref):
    me = lax.axis_index("station")
    for station in range(taken_ref.shape[0]):
        taken_ref[station] = 0

    def place(block, carry):
        distance = routes_ref[block] ^ me
        taken = taken_ref[distance]
        slots_ref[block] = distance * capacity + jnp.minimum(taken, capacity - 1)
        taken_ref[distance] = taken + 1
        return carry

    lax.fori_loop(0, routes_ref.shape[0], place, 0)


def shards(beam_first, beam_second, green_smooth, green_slope, destination):
    resident = beam_first[0, 0]
    opposing = (beam_second[0, 0],)
    groups = lax.axis_size("dom")
    stations = lax.axis_size("station")
    count = resident.shape[1]
    block_count = count // BLOCK
    capacity = max(2, 2 * block_count // stations)
    scale = STRENGTH * GRID * GRID / (count * groups)
    half, whole = array(2, count), array(4, count)
    density = array(GRID, GRID)
    shares = (density, array(GRID, GRID, dtype=jnp.bfloat16))
    table = array(2 * GRID, GRID, dtype=jnp.bfloat16)
    vmem, smem = (pl.BlockSpec(memory_space=space) for space in (pltpu.VMEM, pltpu.SMEM))
    resident, *opposing, kept, sent = local(
        first_kernel,
        (whole, whole, *shares),
        in_specs=[pl.BlockSpec(memory_space=pltpu.HBM)] * 2,
        out_specs=(vmem,) * 4,
        scratch_shapes=[pltpu.SemaphoreType.DMA((2,))],
    )(*(pltpu.with_memory_space_constraint(value, pltpu.HBM) for value in (resident, opposing[0])))
    wide = array(GRID, 3 * GRID, dtype=jnp.bfloat16)
    smooth, slope = local(greens_kernel, (wide, wide))(green_smooth, green_slope)

    def both_tables(kept, sent):
        total = summed(kept, sent, "dom")
        own = local(functools.partial(table_kernel, scale), table)(total, smooth, slope)
        return own, paired(own, "dom", 1)

    place = local(
        functools.partial(slots_kernel, capacity),
        array(block_count, dtype=jnp.int32),
        in_specs=[smem],
        out_specs=smem,
        scratch_shapes=[pltpu.SMEM((stations,), jnp.int32)],
    )(destination[0, :, 0])
    pair = both_tables(kept, sent)
    for _ in range(FRONTS - 1):
        positions, moments = local(opposing_kernel, (half, half))(*pair, *opposing)
        positions = shifted(positions, "station", 1)
        moments = shifted(moments, "station", 1)
        opposing = (positions, moments)
        resident, part = local(resident_kernel, (whole, density))(*pair, resident)
        kept, sent = local(arrival_kernel, shares)(positions, part)
        pair = both_tables(kept, sent)
    blocks = array(capacity, 4, BLOCK)
    parts = local(
        last_kernel,
        (blocks,) * stations,
        in_specs=[smem] + [vmem] * 3,
        out_specs=(vmem,) * stations,
        scratch_shapes=[
            pltpu.VMEM((4, count), jnp.float32),
            pltpu.VMEM((stations * capacity, 4, BLOCK), jnp.float32),
        ],
    )(place, *pair, resident)
    parts = [
        lax.ppermute(part, "station", [(source, source ^ distance) for source in range(stations)])
        if distance
        else part
        for distance, part in enumerate(parts)
    ]
    opposing = local(final_kernel, whole)(*pair, *opposing)
    arrived = local(
        gather_kernel,
        array(stations, capacity, 4, BLOCK),
        in_specs=[vmem] * stations,
        out_specs=pl.BlockSpec(memory_space=pltpu.HBM),
        scratch_shapes=[pltpu.SemaphoreType.DMA((stations,))],
    )(*parts)
    return (arrived[None, None], opposing[None, None])


def solution(mesh):
    placed = (
        P("station", "dom", None, None),
        P("station", "dom", None, None),
        P(),
        P(),
        P("station", "dom", None),
    )
    return jax.shard_map(
        shards,
        mesh=mesh,
        in_specs=placed,
        out_specs=(P("station", "dom", None, None, None, None), P("station", "dom", None, None)),
        check_vma=False,
    )
```

```python
import functools

import jax
import jax.numpy as jnp
from jax import lax
from jax.experimental import pallas as pl
from jax.experimental.pallas import tpu as pltpu
from jax.sharding import PartitionSpec as P


GRID = 128
FRONTS = 4
BLOCK = 128
TILE = 2048
LINES = 8


EDGE = 4.0
DRIFT = 0.05
STRENGTH = 0.06
HIGH = lax.Precision.HIGHEST
SPACING = 2.0 * EDGE / (GRID - 1)


def shifted(value, axis, steps):
    count = lax.axis_size(axis)
    pairs = [(source, (source + steps) % count) for source in range(count)]
    return lax.ppermute(value, axis, pairs)


def paired(value, axis, distance):
    pairs = [(source, source ^ distance) for source in range(lax.axis_size(axis))]
    return lax.ppermute(value, axis, pairs)


def summed(kept, sent, axis):
    value = kept + paired(sent, axis, 1).astype(jnp.float32)
    sent = value.astype(jnp.bfloat16)
    far = [paired(sent, axis, distance) for distance in range(2, lax.axis_size(axis), 2)]
    return value + sum(part.astype(jnp.float32) for part in reversed(far))


def cells(coordinate):
    place = jnp.clip((coordinate + EDGE) * (1.0 / SPACING), -2.0, GRID + 2.0)
    cell = jnp.floor(place)
    upper = place - cell
    lower = 1.0 - upper
    odd = jnp.floor(cell * 0.5)
    even = cell - odd
    is_even = even == odd
    return (even, jnp.where(is_even, lower, upper)), (odd, jnp.where(is_even, upper, lower))


def hat_table(coordinate):
    count = coordinate.shape[1]
    none = jnp.zeros((2 * LINES, count), jnp.bfloat16)
    index = lax.broadcasted_iota(jnp.int32, none.shape, 0).astype(jnp.float32)
    parts = []
    for pair in cells(coordinate):
        cell, weight = (jnp.concatenate([row, row], axis=0).astype(jnp.bfloat16) for row in pair)
        for start in range(0, GRID // 2, 2 * LINES):
            at = (index + float(start)).astype(jnp.bfloat16)
            parts.append(jnp.where(cell == at, weight, none))
    return jnp.concatenate(parts, axis=0)


def deposit(x, y):
    return lax.dot_general(
        hat_table(y), hat_table(x), (((1,), (1,)), ((), ())), preferred_element_type=jnp.float32
    )


def kick(x, moment_x, y, moment_y, table):
    sampled = jnp.dot(table, hat_table(x), preferred_element_type=jnp.float32)
    index = lax.broadcasted_iota(jnp.int32, x.shape, 0).astype(jnp.float32)
    moments = [moment_x, moment_y]
    pushes = [0.0, 0.0]
    block = 0
    for cell, weight in cells(y):
        weight = weight.astype(jnp.bfloat16).astype(jnp.float32)
        found = [jnp.zeros(x.shape, jnp.float32)] * 2
        for start in range(0, GRID // 2, LINES):
            here = cell == index + float(start)
            for which in range(2):
                part = sampled[block * LINES : (block + 1) * LINES]
                found[which] = jnp.where(here, part, found[which])
                block += 1
        pushes = [push + weight * part for push, part in zip(pushes, found)]
    for which, push in enumerate(pushes):
        shift = LINES // 2
        while shift:
            push = push + pltpu.roll(push, shift, 0)
            shift //= 2
        moments[which] = moments[which] - push
    moment_x, moment_y = moments
    return x + DRIFT * moment_x, moment_x, y + DRIFT * moment_y, moment_y


def halves(value):
    high = value.astype(jnp.bfloat16)
    return high, (value - high.astype(jnp.float32)).astype(jnp.bfloat16)


def table_of(density, smooth, slope, scale):
    high, low = halves(density * scale)
    inner = lax.dot_general(
        jnp.concatenate([high, low, high], axis=1),
        jnp.concatenate([slope, smooth], axis=0),
        (((1,), (1,)), ((), ())),
        preferred_element_type=jnp.float32,
    )
    pushes = []
    for which, green in enumerate((smooth, slope)):
        high, low = halves(inner[:, which * GRID : (which + 1) * GRID])
        right = jnp.concatenate([high, low, high], axis=0)
        pushes.append(jnp.dot(green, right, preferred_element_type=jnp.float32))
    return jnp.concatenate(
        [push[start : start + LINES] for start in range(0, GRID, LINES) for push in pushes], axis=0
    ).astype(jnp.bfloat16)


def greens_kernel(smooth_ref, slope_ref, *outs):
    row = lax.broadcasted_iota(jnp.int32, (GRID, GRID), 0)
    column = lax.broadcasted_iota(jnp.int32, (GRID, GRID), 1)
    chosen = jnp.where(row < GRID // 2, 2 * row, 2 * row - (GRID - 1))
    order = (column == chosen).astype(jnp.float32)
    for ref, out_ref in zip((smooth_ref, slope_ref), outs):
        moved = jnp.dot(order, ref[...], precision=HIGH, preferred_element_type=jnp.float32)
        moved = lax.dot_general(
            moved, order, (((1,), (1,)), ((), ())), precision=HIGH, preferred_element_type=jnp.float32
        )
        high, low = halves(moved)
        for place, part in enumerate((high, high, low)):
            out_ref[:, place * GRID : (place + 1) * GRID] = part


def columns(count):
    width = min(TILE, count)
    return [pl.ds(start, width) for start in range(0, count, width)]


def share(resident, opposing):
    even = lax.rem(lax.axis_index("dom"), 2) == 0
    return jnp.where(even, resident, opposing), jnp.where(even, opposing, resident).astype(jnp.bfloat16)


def chosen(which, own_ref, other_ref):
    own = lax.rem(lax.axis_index("dom"), 2) == which
    return jnp.where(own, own_ref[...], other_ref[...])


def first_kernel(resident_hbm, opposing_hbm, resident_ref, opposing_ref, kept_ref, sent_ref, landed):
    held = (resident_ref, opposing_ref)
    copies = [
        pltpu.make_async_copy(source, place, landed.at[which])
        for which, (source, place) in enumerate(zip((resident_hbm, opposing_hbm), held))
    ]
    for copy in copies:
        copy.start()
    densities = []
    for copy in copies:
        copy.wait()
    for beam in held:
        densities.append(
            sum(deposit(line(beam, 0, tile), line(beam, 2, tile)) for tile in columns(beam.shape[1]))
        )
    kept_ref[...], sent_ref[...] = share(*densities)


def line(ref, row, tile):
    return jnp.broadcast_to(ref[row : row + 1, tile], (LINES, tile.size))


def rows(ref, tile):
    return [line(ref, row, tile) for row in range(4)]


def table_kernel(scale, density_ref, smooth_ref, slope_ref, table_ref):
    table_ref[...] = table_of(density_ref[...], smooth_ref[...], slope_ref[...], scale)


def beam_kernel(which, own_ref, other_ref, beam_ref, moved_ref, density_ref):
    table = chosen(which, own_ref, other_ref)
    total = 0.0
    for tile in columns(beam_ref.shape[1]):
        new = kick(*rows(beam_ref, tile), table)
        for row in range(4):
            moved_ref[row : row + 1, tile] = new[row][:1]
        total = total + deposit(new[0], new[2])
    density_ref[...] = total.astype(density_ref.dtype)


def last_kernel(slots_ref, own_ref, other_ref, beam_ref, *refs):
    *packed, moved_ref, slots_out = refs
    table = chosen(1, own_ref, other_ref)
    slots_out[...] = jnp.zeros_like(slots_out)
    for tile in columns(beam_ref.shape[1]):
        new = kick(*rows(beam_ref, tile), table)
        for row in range(4):
            moved_ref[row : row + 1, tile] = new[row][:1]
    for block in range(beam_ref.shape[1] // BLOCK):
        slots_out[slots_ref[block]] = moved_ref[:, block * BLOCK : (block + 1) * BLOCK]
    for distance, ref in enumerate(packed):
        capacity = ref.shape[0]
        ref[...] = slots_out[distance * capacity : (distance + 1) * capacity]


def final_kernel(own_ref, other_ref, beam_ref, out_ref):
    table = chosen(0, own_ref, other_ref)
    for tile in columns(beam_ref.shape[1]):
        new = kick(*rows(beam_ref, tile), table)
        for row in range(4):
            out_ref[row : row + 1, tile] = new[row][:1]


def gather_kernel(*refs):
    *parts, out_hbm, landed = refs
    me = lax.axis_index("station")
    copies = [
        pltpu.make_async_copy(part, out_hbm.at[me ^ distance], landed.at[distance])
        for distance, part in enumerate(parts)
    ]
    for copy in copies:
        copy.start()
    for copy in copies:
        copy.wait()


def local(kernel, out_shape, **options):
    return pl.pallas_call(
        kernel,
        out_shape=out_shape,
        compiler_params=pltpu.CompilerParams(vmem_limit_bytes=24 << 20),
        **options,
    )


def array(*shape, dtype=jnp.float32):
    return jax.ShapeDtypeStruct(shape, dtype)


def slots_kernel(capacity, routes_ref, slots_ref, taken_ref):
    me = lax.axis_index("station")
    for station in range(taken_ref.shape[0]):
        taken_ref[station] = 0

    def place(block, carry):
        distance = routes_ref[block] ^ me
        taken = taken_ref[distance]
        slots_ref[block] = distance * capacity + jnp.minimum(taken, capacity - 1)
        taken_ref[distance] = taken + 1
        return carry

    lax.fori_loop(0, routes_ref.shape[0], place, 0)


def shards(beam_first, beam_second, green_smooth, green_slope, destination):
    resident = beam_first[0, 0]
    opposing = beam_second[0, 0]
    groups = lax.axis_size("dom")
    stations = lax.axis_size("station")
    count = resident.shape[1]
    block_count = count // BLOCK
    capacity = max(2, 2 * block_count // stations)
    scale = STRENGTH * GRID * GRID / (count * groups)
    whole = array(4, count)
    density, rounded = array(GRID, GRID), array(GRID, GRID, dtype=jnp.bfloat16)
    table = array(2 * GRID, GRID, dtype=jnp.bfloat16)
    vmem, smem = (pl.BlockSpec(memory_space=space) for space in (pltpu.VMEM, pltpu.SMEM))
    resident, opposing, kept, sent = local(
        first_kernel,
        (whole, whole, density, rounded),
        in_specs=[pl.BlockSpec(memory_space=pltpu.HBM)] * 2,
        out_specs=(vmem,) * 4,
        scratch_shapes=[pltpu.SemaphoreType.DMA((2,))],
    )(*(pltpu.with_memory_space_constraint(value, pltpu.HBM) for value in (resident, opposing)))
    wide = array(GRID, 3 * GRID, dtype=jnp.bfloat16)
    smooth, slope = local(greens_kernel, (wide, wide))(green_smooth, green_slope)

    def both_tables(kept, sent):
        total = summed(kept, sent, "dom")
        own = local(functools.partial(table_kernel, scale), table)(total, smooth, slope)
        return own, paired(own, "dom", 1)

    place = local(
        functools.partial(slots_kernel, capacity),
        array(block_count, dtype=jnp.int32),
        in_specs=[smem],
        out_specs=smem,
        scratch_shapes=[pltpu.SMEM((stations,), jnp.int32)],
    )(destination[0, :, 0])
    pair = both_tables(kept, sent)
    for _ in range(FRONTS - 1):
        opposing, part = local(functools.partial(beam_kernel, 0), (whole, rounded))(*pair, opposing)
        part = shifted(part, "station", 1)
        opposing = shifted(opposing, "station", 1)
        resident, total = local(functools.partial(beam_kernel, 1), (whole, density))(
            *pair, resident
        )
        pair = both_tables(*share(total, part.astype(jnp.float32)))
    blocks = array(capacity, 4, BLOCK)
    parts = local(
        last_kernel,
        (blocks,) * stations,
        in_specs=[smem] + [vmem] * 3,
        out_specs=(vmem,) * stations,
        scratch_shapes=[
            pltpu.VMEM((4, count), jnp.float32),
            pltpu.VMEM((stations * capacity, 4, BLOCK), jnp.float32),
        ],
    )(place, *pair, resident)
    parts = [
        lax.ppermute(part, "station", [(source, source ^ distance) for source in range(stations)])
        if distance
        else part
        for distance, part in enumerate(parts)
    ]
    opposing = local(final_kernel, whole)(*pair, opposing)
    arrived = local(
        gather_kernel,
        array(stations, capacity, 4, BLOCK),
        in_specs=[vmem] * stations,
        out_specs=pl.BlockSpec(memory_space=pltpu.HBM),
        scratch_shapes=[pltpu.SemaphoreType.DMA((stations,))],
    )(*parts)
    return (arrived[None, None], opposing[None, None])


def solution(mesh):
    placed = (
        P("station", "dom", None, None),
        P("station", "dom", None, None),
        P(),
        P(),
        P("station", "dom", None),
    )
    return jax.shard_map(
        shards,
        mesh=mesh,
        in_specs=placed,
        out_specs=(P("station", "dom", None, None, None, None), P("station", "dom", None, None)),
        check_vma=False,
    )
```

```python
import functools

import jax
import jax.numpy as jnp
from jax import lax
from jax.experimental import pallas as pl
from jax.experimental.pallas import tpu as pltpu
from jax.sharding import PartitionSpec as P


GRID = 128
FRONTS = 4
BLOCK = 128
TILE = 2048
LINES = 8


EDGE = 4.0
DRIFT = 0.05
STRENGTH = 0.06
HIGH = lax.Precision.HIGHEST
SPACING = 2.0 * EDGE / (GRID - 1)


def shifted(value, axis, steps):
    count = lax.axis_size(axis)
    pairs = [(source, (source + steps) % count) for source in range(count)]
    return lax.ppermute(value, axis, pairs)


def crossed(value):
    stations, groups = lax.axis_size("station"), lax.axis_size("dom")
    pairs = [
        (station * groups + index, (station + 1) % stations * groups + (index ^ 1))
        for station in range(stations)
        for index in range(groups)
    ]
    return lax.ppermute(value, ("station", "dom"), pairs)


def paired(value, axis, distance):
    pairs = [(source, source ^ distance) for source in range(lax.axis_size(axis))]
    return lax.ppermute(value, axis, pairs)


def across(chip):
    return 2 * chip + chip % 2


def summed(kept, sent, axis):
    value = kept + paired(sent, axis, 1).astype(jnp.float32)
    sent = value.astype(jnp.bfloat16)
    chips = lax.axis_size(axis) // 2
    far = [paired(sent, axis, across(chip)) for chip in range(1, chips)]
    return value + sum(part.astype(jnp.float32) for part in reversed(far))


def cells(coordinate):
    place = jnp.clip((coordinate + EDGE) * (1.0 / SPACING), -2.0, GRID + 2.0)
    cell = jnp.floor(place)
    upper = place - cell
    lower = 1.0 - upper
    odd = jnp.floor(cell * 0.5)
    even = cell - odd
    is_even = even == odd
    return (even, jnp.where(is_even, lower, upper)), (odd, jnp.where(is_even, upper, lower))


def hat_table(coordinate):
    count = coordinate.shape[1]
    none = jnp.zeros((2 * LINES, count), jnp.bfloat16)
    index = lax.broadcasted_iota(jnp.int32, none.shape, 0).astype(jnp.float32)
    parts = []
    for pair in cells(coordinate):
        cell, weight = (jnp.concatenate([row, row], axis=0).astype(jnp.bfloat16) for row in pair)
        for start in range(0, GRID // 2, 2 * LINES):
            at = (index + float(start)).astype(jnp.bfloat16)
            parts.append(jnp.where(cell == at, weight, none))
    return jnp.concatenate(parts, axis=0)


def deposit(x, y):
    return lax.dot_general(
        hat_table(y), hat_table(x), (((1,), (1,)), ((), ())), preferred_element_type=jnp.float32
    )


def kick(x, moment_x, y, moment_y, table):
    sampled = jnp.dot(table, hat_table(x), preferred_element_type=jnp.float32)
    index = lax.broadcasted_iota(jnp.int32, x.shape, 0).astype(jnp.float32)
    moments = [moment_x, moment_y]
    pushes = [0.0, 0.0]
    block = 0
    for cell, weight in cells(y):
        weight = weight.astype(jnp.bfloat16).astype(jnp.float32)
        found = [jnp.zeros(x.shape, jnp.float32)] * 2
        for start in range(0, GRID // 2, LINES):
            here = cell == index + float(start)
            for which in range(2):
                part = sampled[block * LINES : (block + 1) * LINES]
                found[which] = jnp.where(here, part, found[which])
                block += 1
        pushes = [push + weight * part for push, part in zip(pushes, found)]
    for which, push in enumerate(pushes):
        shift = LINES // 2
        while shift:
            push = push + pltpu.roll(push, shift, 0)
            shift //= 2
        moments[which] = moments[which] - push
    moment_x, moment_y = moments
    return x + DRIFT * moment_x, moment_x, y + DRIFT * moment_y, moment_y


def halves(value):
    high = value.astype(jnp.bfloat16)
    return high, (value - high.astype(jnp.float32)).astype(jnp.bfloat16)


def table_of(density, smooth, slope, scale):
    high, low = halves(density * scale)
    inner = lax.dot_general(
        jnp.concatenate([high, low, high], axis=1),
        jnp.concatenate([slope, smooth], axis=0),
        (((1,), (1,)), ((), ())),
        preferred_element_type=jnp.float32,
    )
    pushes = []
    for which, green in enumerate((smooth, slope)):
        high, low = halves(inner[:, which * GRID : (which + 1) * GRID])
        right = jnp.concatenate([high, low, high], axis=0)
        pushes.append(jnp.dot(green, right, preferred_element_type=jnp.float32))
    return jnp.concatenate(
        [push[start : start + LINES] for start in range(0, GRID, LINES) for push in pushes], axis=0
    ).astype(jnp.bfloat16)


def greens_kernel(smooth_ref, slope_ref, *outs):
    row = lax.broadcasted_iota(jnp.int32, (GRID, GRID), 0)
    column = lax.broadcasted_iota(jnp.int32, (GRID, GRID), 1)
    chosen = jnp.where(row < GRID // 2, 2 * row, 2 * row - (GRID - 1))
    order = (column == chosen).astype(jnp.float32)
    for ref, out_ref in zip((smooth_ref, slope_ref), outs):
        moved = jnp.dot(order, ref[...], precision=HIGH, preferred_element_type=jnp.float32)
        moved = lax.dot_general(
            moved, order, (((1,), (1,)), ((), ())), precision=HIGH, preferred_element_type=jnp.float32
        )
        high, low = halves(moved)
        for place, part in enumerate((high, high, low)):
            out_ref[:, place * GRID : (place + 1) * GRID] = part


def columns(count):
    width = min(TILE, count)
    return [pl.ds(start, width) for start in range(0, count, width)]


def keeps():
    index = lax.axis_index("dom")
    return lax.rem(index + index // 2, 2)


def share(resident, opposing):
    even = keeps() == 0
    return jnp.where(even, resident, opposing), jnp.where(even, opposing, resident).astype(jnp.bfloat16)


def chosen(which, own_ref, other_ref):
    own = keeps() == which
    return jnp.where(own, own_ref[...], other_ref[...])


def first_kernel(resident_hbm, opposing_hbm, resident_ref, opposing_ref, kept_ref, sent_ref, landed):
    held = (resident_ref, opposing_ref)
    copies = [
        pltpu.make_async_copy(source, place, landed.at[which])
        for which, (source, place) in enumerate(zip((resident_hbm, opposing_hbm), held))
    ]
    for copy in copies:
        copy.start()
    densities = []
    for copy in copies:
        copy.wait()
    for beam in held:
        densities.append(
            sum(deposit(line(beam, 0, tile), line(beam, 2, tile)) for tile in columns(beam.shape[1]))
        )
    kept_ref[...], sent_ref[...] = share(*densities)


def line(ref, row, tile):
    return jnp.broadcast_to(ref[row : row + 1, tile], (LINES, tile.size))


def rows(ref, tile):
    return [line(ref, row, tile) for row in range(4)]


def table_kernel(scale, density_ref, smooth_ref, slope_ref, table_ref):
    table_ref[...] = table_of(density_ref[...], smooth_ref[...], slope_ref[...], scale)


def beam_kernel(which, own_ref, other_ref, beam_ref, moved_ref, density_ref):
    table = chosen(which, own_ref, other_ref)
    total = 0.0
    for tile in columns(beam_ref.shape[1]):
        new = kick(*rows(beam_ref, tile), table)
        for row in range(4):
            moved_ref[row : row + 1, tile] = new[row][:1]
        total = total + deposit(new[0], new[2])
    density_ref[...] = total.astype(density_ref.dtype)


def last_kernel(slots_ref, own_ref, other_ref, beam_ref, *refs):
    *packed, moved_ref, slots_out = refs
    table = chosen(1, own_ref, other_ref)
    slots_out[...] = jnp.zeros_like(slots_out)
    for tile in columns(beam_ref.shape[1]):
        new = kick(*rows(beam_ref, tile), table)
        for row in range(4):
            moved_ref[row : row + 1, tile] = new[row][:1]
    for block in range(beam_ref.shape[1] // BLOCK):
        slots_out[slots_ref[block]] = moved_ref[:, block * BLOCK : (block + 1) * BLOCK]
    for distance, ref in enumerate(packed):
        capacity = ref.shape[0]
        ref[...] = slots_out[distance * capacity : (distance + 1) * capacity]


def final_kernel(own_ref, other_ref, beam_ref, out_ref):
    table = chosen(0, own_ref, other_ref)
    for tile in columns(beam_ref.shape[1]):
        new = kick(*rows(beam_ref, tile), table)
        for row in range(4):
            out_ref[row : row + 1, tile] = new[row][:1]


def gather_kernel(*refs):
    *parts, out_hbm, landed = refs
    me = lax.axis_index("station")
    copies = [
        pltpu.make_async_copy(part, out_hbm.at[me ^ distance], landed.at[distance])
        for distance, part in enumerate(parts)
    ]
    for copy in copies:
        copy.start()
    for copy in copies:
        copy.wait()


def local(kernel, out_shape, **options):
    return pl.pallas_call(
        kernel,
        out_shape=out_shape,
        compiler_params=pltpu.CompilerParams(vmem_limit_bytes=24 << 20),
        **options,
    )


def array(*shape, dtype=jnp.float32):
    return jax.ShapeDtypeStruct(shape, dtype)


def slots_kernel(capacity, routes_ref, slots_ref, taken_ref):
    me = lax.axis_index("station")
    for station in range(taken_ref.shape[0]):
        taken_ref[station] = 0

    def place(block, carry):
        distance = routes_ref[block] ^ me
        taken = taken_ref[distance]
        slots_ref[block] = distance * capacity + jnp.minimum(taken, capacity - 1)
        taken_ref[distance] = taken + 1
        return carry

    lax.fori_loop(0, routes_ref.shape[0], place, 0)


def shards(beam_first, beam_second, green_smooth, green_slope, destination):
    resident = beam_first[0, 0]
    opposing = beam_second[0, 0]
    groups = lax.axis_size("dom")
    stations = lax.axis_size("station")
    count = resident.shape[1]
    block_count = count // BLOCK
    capacity = max(2, 2 * block_count // stations)
    scale = STRENGTH * GRID * GRID / (count * groups)
    whole = array(4, count)
    density, rounded = array(GRID, GRID), array(GRID, GRID, dtype=jnp.bfloat16)
    table = array(2 * GRID, GRID, dtype=jnp.bfloat16)
    vmem, smem = (pl.BlockSpec(memory_space=space) for space in (pltpu.VMEM, pltpu.SMEM))
    resident, opposing, kept, sent = local(
        first_kernel,
        (whole, whole, density, rounded),
        in_specs=[pl.BlockSpec(memory_space=pltpu.HBM)] * 2,
        out_specs=(vmem,) * 4,
        scratch_shapes=[pltpu.SemaphoreType.DMA((2,))],
    )(*(pltpu.with_memory_space_constraint(value, pltpu.HBM) for value in (resident, opposing)))
    wide = array(GRID, 3 * GRID, dtype=jnp.bfloat16)
    smooth, slope = local(greens_kernel, (wide, wide))(green_smooth, green_slope)

    def both_tables(kept, sent):
        total = summed(kept, sent, "dom")
        own = local(functools.partial(table_kernel, scale), table)(total, smooth, slope)
        return own, paired(own, "dom", 1)

    place = local(
        functools.partial(slots_kernel, capacity),
        array(block_count, dtype=jnp.int32),
        in_specs=[smem],
        out_specs=smem,
        scratch_shapes=[pltpu.SMEM((stations,), jnp.int32)],
    )(destination[0, :, 0])
    pair = both_tables(kept, sent)
    for _ in range(FRONTS - 1):
        opposing, part = local(functools.partial(beam_kernel, 0), (whole, rounded))(*pair, opposing)
        part = crossed(part)
        opposing = shifted(opposing, "station", 1)
        resident, total = local(functools.partial(beam_kernel, 1), (whole, density))(
            *pair, resident
        )
        pair = both_tables(*share(total, part.astype(jnp.float32)))
    blocks = array(capacity, 4, BLOCK)
    parts = local(
        last_kernel,
        (blocks,) * stations,
        in_specs=[smem] + [vmem] * 3,
        out_specs=(vmem,) * stations,
        scratch_shapes=[
            pltpu.VMEM((4, count), jnp.float32),
            pltpu.VMEM((stations * capacity, 4, BLOCK), jnp.float32),
        ],
    )(place, *pair, resident)
    parts = [
        lax.ppermute(part, "station", [(source, source ^ distance) for source in range(stations)])
        if distance
        else part
        for distance, part in enumerate(parts)
    ]
    opposing = local(final_kernel, whole)(*pair, opposing)
    arrived = local(
        gather_kernel,
        array(stations, capacity, 4, BLOCK),
        in_specs=[vmem] * stations,
        out_specs=pl.BlockSpec(memory_space=pltpu.HBM),
        scratch_shapes=[pltpu.SemaphoreType.DMA((stations,))],
    )(*parts)
    return (arrived[None, None], opposing[None, None])


def solution(mesh):
    placed = (
        P("station", "dom", None, None),
        P("station", "dom", None, None),
        P(),
        P(),
        P("station", "dom", None),
    )
    return jax.shard_map(
        shards,
        mesh=mesh,
        in_specs=placed,
        out_specs=(P("station", "dom", None, None, None, None), P("station", "dom", None, None)),
        check_vma=False,
    )
```

```python
import functools

import jax
import jax.numpy as jnp
from jax import lax
from jax.experimental import pallas as pl
from jax.experimental.pallas import tpu as pltpu
from jax.sharding import PartitionSpec as P


GRID = 128
FRONTS = 4
BLOCK = 128
TILE = 2048
LINES = 8


EDGE = 4.0
DRIFT = 0.05
STRENGTH = 0.06
HIGH = lax.Precision.HIGHEST
SPACING = 2.0 * EDGE / (GRID - 1)


def shifted(value, axis, steps):
    count = lax.axis_size(axis)
    pairs = [(source, (source + steps) % count) for source in range(count)]
    return lax.ppermute(value, axis, pairs)


def crossed(value):
    stations, groups = lax.axis_size("station"), lax.axis_size("dom")
    pairs = [
        (station * groups + index, (station + 1) % stations * groups + (index ^ 1))
        for station in range(stations)
        for index in range(groups)
    ]
    return lax.ppermute(value, ("station", "dom"), pairs)


def paired(value, axis, distance):
    pairs = [(source, source ^ distance) for source in range(lax.axis_size(axis))]
    return lax.ppermute(value, axis, pairs)


def across(chip):
    return 2 * chip + chip // 2 % 2


def summed(kept, sent, axis):
    value = kept + paired(sent, axis, 1).astype(jnp.float32)
    sent = value.astype(jnp.bfloat16)
    chips = lax.axis_size(axis) // 2
    far = [paired(sent, axis, across(chip)) for chip in range(1, chips)]
    return value + sum(part.astype(jnp.float32) for part in reversed(far))


def cells(coordinate):
    place = jnp.clip((coordinate + EDGE) * (1.0 / SPACING), -2.0, GRID + 2.0)
    cell = jnp.floor(place)
    upper = place - cell
    lower = 1.0 - upper
    odd = jnp.floor(cell * 0.5)
    even = cell - odd
    is_even = even == odd
    return (even, jnp.where(is_even, lower, upper)), (odd, jnp.where(is_even, upper, lower))


def hat_table(coordinate):
    count = coordinate.shape[1]
    none = jnp.zeros((2 * LINES, count), jnp.bfloat16)
    index = lax.broadcasted_iota(jnp.int32, none.shape, 0).astype(jnp.float32)
    parts = []
    for pair in cells(coordinate):
        cell, weight = (jnp.concatenate([row, row], axis=0).astype(jnp.bfloat16) for row in pair)
        for start in range(0, GRID // 2, 2 * LINES):
            at = (index + float(start)).astype(jnp.bfloat16)
            parts.append(jnp.where(cell == at, weight, none))
    return jnp.concatenate(parts, axis=0)


def deposit(x, y):
    return lax.dot_general(
        hat_table(y), hat_table(x), (((1,), (1,)), ((), ())), preferred_element_type=jnp.float32
    )


def kick(x, moment_x, y, moment_y, table):
    sampled = jnp.dot(table, hat_table(x), preferred_element_type=jnp.float32)
    index = lax.broadcasted_iota(jnp.int32, x.shape, 0).astype(jnp.float32)
    moments = [moment_x, moment_y]
    pushes = [0.0, 0.0]
    block = 0
    for cell, weight in cells(y):
        weight = weight.astype(jnp.bfloat16).astype(jnp.float32)
        found = [jnp.zeros(x.shape, jnp.float32)] * 2
        for start in range(0, GRID // 2, LINES):
            here = cell == index + float(start)
            for which in range(2):
                part = sampled[block * LINES : (block + 1) * LINES]
                found[which] = jnp.where(here, part, found[which])
                block += 1
        pushes = [push + weight * part for push, part in zip(pushes, found)]
    for which, push in enumerate(pushes):
        shift = LINES // 2
        while shift:
            push = push + pltpu.roll(push, shift, 0)
            shift //= 2
        moments[which] = moments[which] - push
    moment_x, moment_y = moments
    return x + DRIFT * moment_x, moment_x, y + DRIFT * moment_y, moment_y


def halves(value):
    high = value.astype(jnp.bfloat16)
    return high, (value - high.astype(jnp.float32)).astype(jnp.bfloat16)


def table_of(density, smooth, slope, scale):
    high, low = halves(density * scale)
    inner = lax.dot_general(
        jnp.concatenate([high, low, high], axis=1),
        jnp.concatenate([slope, smooth], axis=0),
        (((1,), (1,)), ((), ())),
        preferred_element_type=jnp.float32,
    )
    pushes = []
    for which, green in enumerate((smooth, slope)):
        high, low = halves(inner[:, which * GRID : (which + 1) * GRID])
        right = jnp.concatenate([high, low, high], axis=0)
        pushes.append(jnp.dot(green, right, preferred_element_type=jnp.float32))
    return jnp.concatenate(
        [push[start : start + LINES] for start in range(0, GRID, LINES) for push in pushes], axis=0
    ).astype(jnp.bfloat16)


def greens_kernel(smooth_ref, slope_ref, *outs):
    row = lax.broadcasted_iota(jnp.int32, (GRID, GRID), 0)
    column = lax.broadcasted_iota(jnp.int32, (GRID, GRID), 1)
    chosen = jnp.where(row < GRID // 2, 2 * row, 2 * row - (GRID - 1))
    order = (column == chosen).astype(jnp.float32)
    for ref, out_ref in zip((smooth_ref, slope_ref), outs):
        moved = jnp.dot(order, ref[...], precision=HIGH, preferred_element_type=jnp.float32)
        moved = lax.dot_general(
            moved, order, (((1,), (1,)), ((), ())), precision=HIGH, preferred_element_type=jnp.float32
        )
        high, low = halves(moved)
        for place, part in enumerate((high, high, low)):
            out_ref[:, place * GRID : (place + 1) * GRID] = part


def columns(count):
    width = min(TILE, count)
    return [pl.ds(start, width) for start in range(0, count, width)]


def keeps():
    index = lax.axis_index("dom")
    return lax.rem(index + index // 4, 2)


def share(resident, opposing):
    even = keeps() == 0
    return jnp.where(even, resident, opposing), jnp.where(even, opposing, resident).astype(jnp.bfloat16)


def chosen(which, own_ref, other_ref):
    own = keeps() == which
    return jnp.where(own, own_ref[...], other_ref[...])


def first_kernel(resident_hbm, opposing_hbm, resident_ref, opposing_ref, kept_ref, sent_ref, landed):
    held = (resident_ref, opposing_ref)
    copies = [
        pltpu.make_async_copy(source, place, landed.at[which])
        for which, (source, place) in enumerate(zip((resident_hbm, opposing_hbm), held))
    ]
    for copy in copies:
        copy.start()
    densities = []
    for copy in copies:
        copy.wait()
    for beam in held:
        densities.append(
            sum(deposit(line(beam, 0, tile), line(beam, 2, tile)) for tile in columns(beam.shape[1]))
        )
    kept_ref[...], sent_ref[...] = share(*densities)


def line(ref, row, tile):
    return jnp.broadcast_to(ref[row : row + 1, tile], (LINES, tile.size))


def rows(ref, tile):
    return [line(ref, row, tile) for row in range(4)]


def table_kernel(scale, density_ref, smooth_ref, slope_ref, table_ref):
    table_ref[...] = table_of(density_ref[...], smooth_ref[...], slope_ref[...], scale)


def beam_kernel(which, own_ref, other_ref, beam_ref, moved_ref, density_ref):
    table = chosen(which, own_ref, other_ref)
    total = 0.0
    for tile in columns(beam_ref.shape[1]):
        new = kick(*rows(beam_ref, tile), table)
        for row in range(4):
            moved_ref[row : row + 1, tile] = new[row][:1]
        total = total + deposit(new[0], new[2])
    density_ref[...] = total.astype(density_ref.dtype)


def last_kernel(slots_ref, own_ref, other_ref, beam_ref, *refs):
    *packed, moved_ref, slots_out = refs
    table = chosen(1, own_ref, other_ref)
    slots_out[...] = jnp.zeros_like(slots_out)
    for tile in columns(beam_ref.shape[1]):
        new = kick(*rows(beam_ref, tile), table)
        for row in range(4):
            moved_ref[row : row + 1, tile] = new[row][:1]
    for block in range(beam_ref.shape[1] // BLOCK):
        slots_out[slots_ref[block]] = moved_ref[:, block * BLOCK : (block + 1) * BLOCK]
    for distance, ref in enumerate(packed):
        capacity = ref.shape[0]
        ref[...] = slots_out[distance * capacity : (distance + 1) * capacity]


def final_kernel(own_ref, other_ref, beam_ref, out_ref):
    table = chosen(0, own_ref, other_ref)
    for tile in columns(beam_ref.shape[1]):
        new = kick(*rows(beam_ref, tile), table)
        for row in range(4):
            out_ref[row : row + 1, tile] = new[row][:1]


def gather_kernel(*refs):
    *parts, out_hbm, landed = refs
    me = lax.axis_index("station")
    copies = [
        pltpu.make_async_copy(part, out_hbm.at[me ^ distance], landed.at[distance])
        for distance, part in enumerate(parts)
    ]
    for copy in copies:
        copy.start()
    for copy in copies:
        copy.wait()


def local(kernel, out_shape, **options):
    return pl.pallas_call(
        kernel,
        out_shape=out_shape,
        compiler_params=pltpu.CompilerParams(vmem_limit_bytes=24 << 20),
        **options,
    )


def array(*shape, dtype=jnp.float32):
    return jax.ShapeDtypeStruct(shape, dtype)


def slots_kernel(capacity, routes_ref, slots_ref, taken_ref):
    me = lax.axis_index("station")
    for station in range(taken_ref.shape[0]):
        taken_ref[station] = 0

    def place(block, carry):
        distance = routes_ref[block] ^ me
        taken = taken_ref[distance]
        slots_ref[block] = distance * capacity + jnp.minimum(taken, capacity - 1)
        taken_ref[distance] = taken + 1
        return carry

    lax.fori_loop(0, routes_ref.shape[0], place, 0)


def shards(beam_first, beam_second, green_smooth, green_slope, destination):
    resident = beam_first[0, 0]
    opposing = beam_second[0, 0]
    groups = lax.axis_size("dom")
    stations = lax.axis_size("station")
    count = resident.shape[1]
    block_count = count // BLOCK
    capacity = max(2, 2 * block_count // stations)
    scale = STRENGTH * GRID * GRID / (count * groups)
    whole = array(4, count)
    density, rounded = array(GRID, GRID), array(GRID, GRID, dtype=jnp.bfloat16)
    table = array(2 * GRID, GRID, dtype=jnp.bfloat16)
    vmem, smem = (pl.BlockSpec(memory_space=space) for space in (pltpu.VMEM, pltpu.SMEM))
    resident, opposing, kept, sent = local(
        first_kernel,
        (whole, whole, density, rounded),
        in_specs=[pl.BlockSpec(memory_space=pltpu.HBM)] * 2,
        out_specs=(vmem,) * 4,
        scratch_shapes=[pltpu.SemaphoreType.DMA((2,))],
    )(*(pltpu.with_memory_space_constraint(value, pltpu.HBM) for value in (resident, opposing)))
    wide = array(GRID, 3 * GRID, dtype=jnp.bfloat16)
    smooth, slope = local(greens_kernel, (wide, wide))(green_smooth, green_slope)

    def both_tables(kept, sent):
        total = summed(kept, sent, "dom")
        own = local(functools.partial(table_kernel, scale), table)(total, smooth, slope)
        return own, paired(own, "dom", 1)

    place = local(
        functools.partial(slots_kernel, capacity),
        array(block_count, dtype=jnp.int32),
        in_specs=[smem],
        out_specs=smem,
        scratch_shapes=[pltpu.SMEM((stations,), jnp.int32)],
    )(destination[0, :, 0])
    pair = both_tables(kept, sent)
    for _ in range(FRONTS - 1):
        opposing, part = local(functools.partial(beam_kernel, 0), (whole, rounded))(*pair, opposing)
        part = crossed(part)
        opposing = shifted(opposing, "station", 1)
        resident, total = local(functools.partial(beam_kernel, 1), (whole, density))(
            *pair, resident
        )
        pair = both_tables(*share(total, part.astype(jnp.float32)))
    blocks = array(capacity, 4, BLOCK)
    parts = local(
        last_kernel,
        (blocks,) * stations,
        in_specs=[smem] + [vmem] * 3,
        out_specs=(vmem,) * stations,
        scratch_shapes=[
            pltpu.VMEM((4, count), jnp.float32),
            pltpu.VMEM((stations * capacity, 4, BLOCK), jnp.float32),
        ],
    )(place, *pair, resident)
    parts = [
        paired(part, "station", distance) if distance else part
        for distance, part in enumerate(parts)
    ]
    opposing = local(final_kernel, whole)(*pair, opposing)
    arrived = local(
        gather_kernel,
        array(stations, capacity, 4, BLOCK),
        in_specs=[vmem] * stations,
        out_specs=pl.BlockSpec(memory_space=pltpu.HBM),
        scratch_shapes=[pltpu.SemaphoreType.DMA((stations,))],
    )(*parts)
    return (arrived[None, None], opposing[None, None])


def solution(mesh):
    placed = (
        P("station", "dom", None, None),
        P("station", "dom", None, None),
        P(),
        P(),
        P("station", "dom", None),
    )
    return jax.shard_map(
        shards,
        mesh=mesh,
        in_specs=placed,
        out_specs=(P("station", "dom", None, None, None, None), P("station", "dom", None, None)),
        check_vma=False,
    )
```
